32 devices in a mesh: kern: 16 (over z, y, x), walk: 2 (over core).
Axes of the slice: x: 2, y: 2, z: 4, core: 2. Of those that a mesh axis runs over, the one named last changes fastest.
Arguments:
- walkers: float32 [8, 2048], P(None, 'walk'), may hold values from -5 to 5
- centers: float32 [8, 32768], P(None, 'kern'), may hold values from -5 to 5
- sigmas: float32 [8, 32768], P(None, 'kern'), may hold values from 0.6 to 1.5
- heights: float32 [32768], P('kern'), may hold values from 0.2 to 2
- kernel_live: int32 [16], P('kern'), may hold values from 512 to 2048, as said below
- merge_target: int32 [2048], P('walk'), may hold values from 0 to 32767, as said below
- new_sigma: float32 [8], replicated, may hold values from 0.2 to 0.6
- norm_old: float32 [1], replicated, may hold values from 0.003 to 0.03
Outputs:
- bias: float32 [2048], P('walk')
- force: float32 [8, 2048], P(None, 'walk')
- new_heights: float32 [32768], P('kern')
- new_centers: float32 [8, 32768], P(None, 'kern')
- new_sigmas: float32 [8, 32768], P(None, 'kern')
- log_norm: float32 [1], replicated
The draws below stay inside these ranges and needn't reach their ends.
Inputs may be any that keep to these rules, and one draw needn't show every extreme that they name: `kernel_live`: slots from this number up are empty; some shard is full in every draw. `merge_target`: each entry is shard * 2048 + slot with slot below that shard's kernel_live; among the 1024 walkers of one index of walk at most 128 target one shard, every shard is targeted, and some shard receives exactly 128 in every block.
All inputs are finite; a program needn't handle non-finite values.
Results may differ from the reference program's by a relative error of at most 0.0003.
Values sent between devices are 32-bit elements; how exact they have to be, the bound alone decides.
A program may use at most 64 MiB of HBM per device.

```python
import math
import jax
import jax.numpy as jnp
from jax import lax

DIMS = 8
KS = 2048
WB = 1024
KERNELS = 32768
WALKERS = 2048
N_KERN = 16
N_WALK = 2


def live_table(key):
    first, second = jax.random.split(jax.random.fold_in(key, 11))
    live_count = jax.random.randint(first, (N_KERN,), KS // 4, KS + 1)
    fullest = jax.random.randint(second, (), 0, N_KERN)
    return jnp.where(jnp.arange(N_KERN) == fullest, KS, live_count).astype(jnp.int32)


def draw_kernel_live(key, part):
    return live_table(key)


def block_shards(block_key):
    capacity = 2 * WB // N_KERN
    key_busy, key_pick, key_order = jax.random.split(block_key, 3)
    busiest = jax.random.randint(key_busy, (), 0, N_KERN)
    others = (busiest + 1 + jnp.arange(N_KERN - 1)) % N_KERN
    units = (N_KERN - 1) * (capacity - 1)
    extra = WB - capacity - (N_KERN - 1)
    picked = jax.random.permutation(key_pick, units)[:extra]
    listed = jnp.concatenate([jnp.full((capacity,), busiest), others, others[picked // (capacity - 1)]])
    return jax.random.permutation(key_order, listed)


def draw_merge_target(key, part):
    live_count = live_table(key)
    block_keys = jax.random.split(jax.random.fold_in(key, 31), N_WALK)
    shards = jax.vmap(block_shards)(block_keys).reshape(-1)
    raw_slot = jax.random.randint(jax.random.fold_in(key, 47), (WALKERS,), 0, 1 << 30)
    slot = raw_slot % live_count[shards]
    return (shards * KS + slot).astype(jnp.int32)


def levels(rng, dims, cuts, smallest, top_value):
    def one(axis_at, shards_of):
        steps = jax.random.uniform(jax.random.fold_in(jax.random.fold_in(rng, 6), axis_at), (shards_of,), jnp.float32, smallest / len(cuts), top_value / len(cuts))
        return jnp.repeat(jnp.exp(steps), dims[axis_at] // shards_of).reshape((-1,) + (1,) * (len(dims) - axis_at - 1))

    gain = one(*cuts[0])
    for cut in cuts[1:]:
        gain = gain * one(*cut)
    return gain


def noise(own_key, shape, spread, bound, cuts=(), kind=jnp.bfloat16):
    loudness = levels(own_key, shape, cuts, -0.22, 0.18) if cuts else 1.0
    values = jax.random.normal(own_key, shape, jnp.float32) * spread * loudness
    return jnp.minimum(jnp.maximum(values, -bound), bound).astype(kind)


def setup_inputs(seed: int = 0) -> dict:
    key_of = jax.random.split(jax.random.key(seed), 9)
    return {
        "walkers": noise(key_of[0], (DIMS, WALKERS), 1.0, 5.0, ((1, 2),), jnp.float32),
        "centers": noise(key_of[1], (DIMS, KERNELS), 1.0, 5.0, ((1, 16),), jnp.float32),
        "sigmas": jnp.clip(jnp.exp(math.log(1.5) - 0.9162907 * jax.random.uniform(key_of[2], (DIMS, KERNELS), jnp.float32) ** levels(key_of[2], (DIMS, KERNELS), ((1, 16),), -0.2, 0.2)), 0.6, 1.5),
        "heights": jnp.clip(jnp.exp(math.log(2.0) - 2.3025851 * jax.random.uniform(key_of[3], (KERNELS,), jnp.float32) ** levels(key_of[3], (KERNELS,), ((0, 16),), -0.2, 0.2)), 0.2, 2.0),
        "kernel_live": draw_kernel_live(jax.random.fold_in(key_of[8], 71), 0),
        "merge_target": draw_merge_target(jax.random.fold_in(key_of[8], 71), 0),
        "new_sigma": jnp.clip(jnp.exp(jax.random.uniform(key_of[6], (DIMS,), jnp.float32, math.log(0.2), math.log(0.6))), 0.2, 0.6),
        "norm_old": jnp.clip(jnp.exp(jax.random.uniform(key_of[7], (1,), jnp.float32, math.log(0.003), math.log(0.03))), 0.003, 0.03),
    }


PREFACTOR = 0.9
EPSILON = 0.01
RATE = 0.25

def reference(walkers, centers, sigmas, heights, kernel_live, merge_target, new_sigma, norm_old):
    inverse_var = 1.0 / (sigmas * sigmas)
    slot_of = jnp.arange(KERNELS, dtype=jnp.int32) % KS
    alive = (slot_of < jnp.repeat(kernel_live, KS)).astype(jnp.float32)
    kernel_feat = jnp.concatenate([-0.5 * inverse_var, centers * inverse_var, (jnp.log(heights) - 0.5 * lax.optimization_barrier(jnp.sum(centers * centers * inverse_var, 0)))[None]], 0)
    kernel_mom = jnp.concatenate([alive[None], inverse_var * alive, centers * inverse_var * alive], 0)
    walker_feat = jnp.concatenate([walkers * walkers, walkers, jnp.ones((1, WALKERS), jnp.float32)], 0)
    block_len = 1024 if KERNELS % 1024 == 0 else KS
    block_count = KERNELS // block_len

    def step(running, block_index):
        start = (block_index * block_len).astype(jnp.int32)
        feat = lax.dynamic_slice_in_dim(kernel_feat, start, block_len, 1)
        moms = lax.dynamic_slice_in_dim(kernel_mom, start, block_len, 1)
        expo = lax.dot_general(feat, walker_feat, (((0,), (0,)), ((), ())), precision=lax.Precision.HIGHEST)
        return (running + jnp.dot(moms, jnp.exp(expo), precision=lax.Precision.HIGHEST), None)
    moments, _ = lax.scan(step, jnp.zeros((17, WALKERS), jnp.float32), jnp.arange(block_count, dtype=jnp.int32))
    live_total = jnp.sum(kernel_live).astype(jnp.float32)
    density = moments[0] / live_total
    grad = (-walkers * moments[1:9] + moments[9:17]) / live_total
    norm_value = norm_old[0]
    ratio = density / norm_value + EPSILON
    bias = PREFACTOR * jnp.log(ratio)
    force = -PREFACTOR * grad / (norm_value * ratio)
    weight = jnp.exp(bias)
    log_norm = jnp.log((1.0 - RATE) * norm_old + RATE * jnp.sum(density) / WALKERS)
    target_center = centers[:, merge_target]
    offset = walkers - target_center
    feat = jnp.concatenate([weight[None], weight * offset, weight * (offset * offset + (new_sigma * new_sigma)[:, None])], 0)
    merged_sums = jax.ops.segment_sum(feat.T, merge_target, KERNELS).T
    new_heights = heights + merged_sums[0]
    delta = merged_sums[1:9] / new_heights
    new_centers = centers + delta
    new_sigmas = jnp.sqrt((heights * sigmas * sigmas + merged_sums[9:17]) / new_heights - delta * delta)
    return (bias, force, new_heights, new_centers, new_sigmas, log_norm)
```

```python
import functools
import math

import jax
import jax.numpy as jnp
from jax import lax
from jax.experimental import pallas as pl
from jax.experimental.pallas import tpu as pltpu
from jax.sharding import PartitionSpec as P

PREFACTOR = 0.9
EPSILON = 0.01
RATE = 0.25
LANES = 128
LOG2E = math.log2(math.e)
MESH = pl.DeviceIdType.MESH
F32 = jnp.float32
BF16 = jnp.bfloat16
VMEM = pl.BlockSpec(memory_space=pltpu.VMEM)
HBM = pl.BlockSpec(memory_space=pltpu.HBM)
LIMIT = 24 << 20


def split(x):
    high = x.astype(BF16).astype(F32)
    rest = x - high
    middle = rest.astype(BF16).astype(F32)
    low = (rest - middle).astype(BF16).astype(F32)
    return high, middle, low


def row_of(parts, width):
    row = lax.broadcasted_iota(jnp.int32, (8, width), 0)
    block = jnp.zeros((8, width), F32)
    for index, part in enumerate(parts):
        block = jnp.where(row == index, part, block)
    return block


def farthest_first(count):
    return sorted(range(count), key=lambda step: -min(step, count - step))


def sums_kernel(kern_count, walk_count, groups, capacity,
                walkers_hbm, target_hbm, centers_hbm, sigmas_hbm, heights_hbm, live_hbm, norm_hbm, new_sigma_hbm,
                bias_ref, force_ref, new_heights_ref, new_centers_ref, new_sigmas_ref, log_norm_ref,
                walkers_ref, target_ref, centers_ref, sigmas_ref, heights_ref, live_ref, norm_ref, new_sigma_ref, load_sem,
                walker_feat, kernel_feat, kernel_mom, sums, own, got, mine, shared, far,
                far_walkers, far_targets, table, placing,
                send_a, recv_a, send_b, recv_b, send_c, recv_c, send_w, recv_w, send_t, recv_t):
    loads = [
        pltpu.make_async_copy(source, target, load_sem.at[index])
        for index, (source, target) in enumerate(
            [
                (walkers_hbm, walkers_ref),
                (centers_hbm, centers_ref),
                (sigmas_hbm, sigmas_ref),
                (heights_hbm, heights_ref),
                (live_hbm, live_ref),
                (norm_hbm, norm_ref),
                (target_hbm, target_ref),
                (new_sigma_hbm, new_sigma_ref),
            ]
        )
    ]
    for load in loads:
        load.start()
    dims, walk_len = walkers_ref.shape
    shard_len = centers_ref.shape[1]
    per = dims // groups
    chunks = kern_count // groups
    me = lax.axis_index("kern")
    walk = lax.axis_index("walk")
    my_chunk = me // groups
    my_group = lax.rem(me, groups)

    def biased(density):
        return PREFACTOR * jnp.log(density / norm + EPSILON)

    def peer(step):
        return lax.rem(me + step, kern_count)

    def other(step):
        return lax.rem(walk + step, walk_count)

    def far_kern(index):
        return index * groups + my_group

    barrier = pltpu.get_barrier_semaphore()

    def greet(step, carry):
        pl.semaphore_signal(barrier, inc=1, device_id=(peer(step), walk), device_id_type=MESH)
        return carry

    lax.fori_loop(1, kern_count, greet, 0)
    for step in range(1, walk_count):
        def greet_far(index, carry):
            pl.semaphore_signal(
                barrier, inc=1, device_id=(far_kern(index), other(step)), device_id_type=MESH
            )
            return carry

        lax.fori_loop(0, chunks, greet_far, 0)

    for load in loads:
        load.wait()
    norm = norm_ref[0]
    walkers = walkers_ref[...]
    sq_h, sq_m, sq_l = split(walkers * walkers)
    wk_h, wk_m, wk_l = split(walkers)
    h, m, l = [sq_h, wk_h], [sq_m, wk_m], [sq_l, wk_l]
    one = jnp.ones((1, walk_len), F32)
    pad = jnp.zeros((LANES - 12 * dims - 8, walk_len), F32)
    stacked = jnp.concatenate(h + m + h + m + l + h + [row_of([one] * 3, walk_len), pad], 0)
    stacked = stacked.astype(BF16)
    width = 2 * LANES
    quarters = walk_len // width
    for quarter in range(quarters):
        walker_feat[quarter] = stacked[:, quarter * width : (quarter + 1) * width]

    centers = centers_ref[...]
    sigmas = sigmas_ref[...]
    inverse_var = 1.0 / (sigmas * sigmas)
    scaled = centers * inverse_var
    constant = jnp.log(heights_ref[...]) - 0.5 * jnp.sum(centers * scaled, 0, keepdims=True)
    k_sq = split((-0.5 * LOG2E) * inverse_var)
    k_lin = split(LOG2E * scaled)
    con = row_of(split(LOG2E * constant), shard_len)
    h, m, l = [[k_sq[i], k_lin[i]] for i in range(3)]
    pad = jnp.zeros((LANES - 12 * dims - 8, shard_len), F32)
    kernel_feat[...] = jnp.concatenate(h + h + m + m + h + l + [con, pad], 0).T.astype(BF16)

    live = live_ref[0]
    alive = (lax.broadcasted_iota(jnp.int32, (8, shard_len), 1) < live).astype(F32)
    mom_a = split(inverse_var * alive)
    mom_c = split(scaled * alive)
    pad = jnp.zeros((8, shard_len), F32)
    rows = [mom_a[0], mom_c[0], mom_a[1], mom_c[1], mom_a[2], mom_c[2], row_of([alive], shard_len), pad]
    kernel_mom[...] = jnp.concatenate(rows, 0).astype(BF16)

    live_row = jnp.full((1, LANES), live, jnp.int32).astype(F32)
    for unit in range(kern_count):
        chunk, group = unit // groups, unit % groups
        own[unit] = walkers[group * per : (group + 1) * per, chunk * LANES : (chunk + 1) * LANES]

    units = kern_count // quarters
    block = min(512, shard_len)

    def copy_a(target, source):
        return pltpu.make_async_remote_copy(
            src_ref=sums.at[target], dst_ref=got.at[source],
            send_sem=send_a.at[target], recv_sem=recv_a.at[source],
            device_id=(target, walk), device_id_type=MESH,
        )

    def compute(step):
        quarter = lax.rem(me // units + step, quarters)
        feat = walker_feat[quarter]
        total = None
        for index in range(shard_len // block):
            part = slice(index * block, (index + 1) * block)
            e = jnp.exp2(jnp.dot(kernel_feat[part, :], feat, preferred_element_type=F32))
            high = e.astype(BF16)
            low = (e - high.astype(F32)).astype(BF16)
            moms = kernel_mom[:, part]
            add = jnp.dot(moms, high, preferred_element_type=F32) + jnp.dot(
                moms, low, preferred_element_type=F32
            )
            total = add if total is None else total + add
        moments = total
        a_sum = moments[0:dims] + moments[2 * dims : 3 * dims] + moments[4 * dims : 5 * dims]
        c_sum = moments[dims : 2 * dims] + moments[3 * dims : 4 * dims] + moments[5 * dims : 6 * dims]
        density = moments[6 * dims : 6 * dims + 1]
        for chunk in range(2):
            part = slice(chunk * LANES, (chunk + 1) * LANES)
            for group in range(groups):
                unit = quarter * units + chunk * groups + group
                rows = slice(group * per, (group + 1) * per)
                sums[unit, 0:per, :] = a_sum[rows, part]
                sums[unit, per : 2 * per, :] = c_sum[rows, part]
                sums[unit, 2 * per : 2 * per + 1, :] = density[:, part]
                sums[unit, 2 * per + 1 : 2 * per + 2, :] = live_row

    def send(step):
        quarter = lax.rem(me // units + step, quarters)

        def start_a(index, carry):
            copy_a(quarter * units + lax.rem(me + index, units), me).start()
            return carry

        lax.fori_loop(0 if step else 1, units, start_a, 0)

    def copy_w(step, source):
        return (
            pltpu.make_async_remote_copy(
                src_ref=walkers_ref, dst_ref=far_walkers.at[source],
                send_sem=send_w.at[step], recv_sem=recv_w.at[source],
                device_id=(me, other(step)), device_id_type=MESH,
            ),
            pltpu.make_async_remote_copy(
                src_ref=target_ref, dst_ref=far_targets.at[source],
                send_sem=send_t.at[step], recv_sem=recv_t.at[source],
                device_id=(me, other(step)), device_id_type=MESH,
            ),
        )

    order = farthest_first(quarters)
    for position, step in enumerate(order):
        compute(step)
        if position == 1:
            pl.semaphore_wait(barrier, kern_count - 1 + (walk_count - 1) * chunks)
            send(order[0])
            for far_step in range(1, walk_count):
                for copy in copy_w(far_step, walk):
                    copy.start()
        if position >= 1:
            send(step)

    got[me] = sums[me]
    def wait_a(step, carry):
        copy_a(peer(step), peer(step)).wait_recv()
        return carry

    lax.fori_loop(1, kern_count, wait_a, 0)
    total = got[0]
    for source in range(1, kern_count):
        total = total + got[source]

    live_total = total[2 * per + 1 : 2 * per + 2]
    density = total[2 * per : 2 * per + 1] / live_total
    grad = (-own[me] * total[0:per] + total[per : 2 * per]) / live_total
    ratio = density / norm + EPSILON
    force = -PREFACTOR * grad / (norm * ratio)
    mine[0:1, :] = density
    mine[1 : per + 1, :] = force

    def copy_b(target, source):
        return pltpu.make_async_remote_copy(
            src_ref=mine, dst_ref=shared.at[source],
            send_sem=send_b.at[target], recv_sem=recv_b.at[source],
            device_id=(target, walk), device_id_type=MESH,
        )

    def copy_c(step, index, chunk, source):
        return pltpu.make_async_remote_copy(
            src_ref=mine, dst_ref=far.at[source, chunk],
            send_sem=send_c.at[step, index], recv_sem=recv_c.at[source, chunk],
            device_id=(far_kern(index), other(step)), device_id_type=MESH,
        )

    def start_b(step, carry):
        copy_b(peer(step), me).start()
        return carry

    for step in range(1, walk_count):
        def start_c(index, carry):
            copy_c(step, lax.rem(my_chunk + index, chunks), my_chunk, walk).start()
            return carry

        half = chunks // 2
        lax.fori_loop(half, chunks, start_c, 0)
        lax.fori_loop(0, half, start_c, 0)
    lax.fori_loop(kern_count // 2, kern_count, start_b, 0)
    lax.fori_loop(1, kern_count // 2, start_b, 0)

    shared[me, 0:1, :] = density
    shared[me, 1 : per + 1, :] = force

    far_walkers[walk] = walkers
    far_targets[walk] = target_ref[...]
    for step in range(1, walk_count):
        for copy in copy_w(step, other(step)):
            copy.wait_recv()
    targets = [far_targets[index] for index in range(walk_count)]
    if walk_count % 8:
        targets.append(jnp.full((8 - walk_count % 8, walk_len), -1, jnp.int32))
    local = jnp.concatenate(targets, 0) - me * shard_len
    owned = (local >= 0) & (local < shard_len)
    before = lax.broadcasted_iota(jnp.int32, (walk_len, walk_len), 0) < lax.broadcasted_iota(
        jnp.int32, (walk_len, walk_len), 1
    )
    place = jnp.dot(
        jnp.where(owned, 1.0, 0.0).astype(BF16),
        jnp.where(before, 1.0, 0.0).astype(BF16),
        preferred_element_type=F32,
    )
    place = jnp.where(owned, place, -1.0)
    slot = jnp.where(owned, (local + 1).astype(F32), 0.0)
    want = lax.broadcasted_iota(jnp.int32, (capacity, walk_len), 0).astype(F32)

    def pack(feat, index):
        return lax.dot_general(
            feat.astype(BF16), table[index], (((1,), (1,)), ((), ())), preferred_element_type=F32
        )

    slots = lax.broadcasted_iota(jnp.int32, (shard_len, capacity), 0).astype(F32)
    packed_walkers = []
    for index in range(walk_count):
        table[index] = jnp.where(want == place[index : index + 1], 1.0, 0.0).astype(BF16)
        high, middle, low = split(far_walkers[index])
        slot_rows = row_of(split(slot[index : index + 1]), walk_len)
        packed = pack(jnp.concatenate([high, middle, low, slot_rows], 0), index)
        packed_walkers.append(packed[0:dims] + (packed[dims : 2 * dims] + packed[2 * dims : 3 * dims]))
        at = 3 * dims
        packed_slot = packed[at : at + 1] + packed[at + 1 : at + 2] + packed[at + 2 : at + 3] - 1.0
        placing[index] = jnp.where(slots == packed_slot, 1.0, 0.0).astype(BF16)

    def wait_b(step, carry):
        copy_b(peer(step), peer(step)).wait_recv()
        return carry

    lax.fori_loop(1, kern_count, wait_b, 0)
    for chunk in range(chunks):
        far[walk, chunk] = shared[chunk * groups]
    for chunk in range(chunks):
        part = slice(chunk * LANES, (chunk + 1) * LANES)
        bias_ref[:, part] = biased(shared[chunk * groups][0:1, :])
        for group in range(groups):
            force_ref[group * per : (group + 1) * per, part] = shared[chunk * groups + group][1 : per + 1, :]
    for step in range(1, walk_count):
        def wait_c(index, carry):
            copy_c(step, index, index, other(step)).wait_recv()
            return carry

        lax.fori_loop(0, chunks, wait_c, 0)
    density_sum = jnp.zeros((1, 1), F32)
    merged = None
    for index in range(walk_count):
        whole = jnp.concatenate([far[index, chunk][0:1, :] for chunk in range(chunks)], 1)
        density_sum = density_sum + jnp.sum(whole, 1, keepdims=True)
        packed = pack(row_of(split(whole), walk_len), index)
        weight = jnp.exp(biased(packed[0:1] + packed[1:2] + packed[2:3]))
        lin = split(weight * packed_walkers[index])
        sq = split(weight * (packed_walkers[index] * packed_walkers[index]))
        last = row_of(split(weight), capacity)
        pad = jnp.zeros((8, capacity), F32)
        feat = jnp.concatenate([lin[0], sq[0], lin[1], sq[1], lin[2], sq[2], last, pad], 0).astype(BF16)
        add = lax.dot_general(feat, placing[index], (((1,), (1,)), ((), ())), preferred_element_type=F32)
        merged = add if merged is None else merged + add
    log_norm_ref[...] = jnp.log((1.0 - RATE) * norm + RATE * density_sum / (walk_len * walk_count))

    first = merged[0:dims] + (merged[2 * dims : 3 * dims] + merged[4 * dims : 5 * dims])
    second = merged[dims : 2 * dims] + (merged[3 * dims : 4 * dims] + merged[5 * dims : 6 * dims])
    at = 6 * dims
    gain = merged[at : at + 1] + (merged[at + 1 : at + 2] + merged[at + 2 : at + 3])
    row = lax.broadcasted_iota(jnp.int32, (dims, dims), 0)
    column = lax.broadcasted_iota(jnp.int32, (dims, dims), 1)
    new_sigma = jnp.sum(jnp.where(row == column, new_sigma_ref[...], 0.0), 1, keepdims=True)
    centers = centers_ref[...]
    sigmas = sigmas_ref[...]
    heights = heights_ref[...]
    shift = first - centers * gain
    spread = second - 2.0 * centers * first + centers * centers * gain + new_sigma * new_sigma * gain
    new_heights = heights + gain
    delta = shift / new_heights
    new_heights_ref[...] = new_heights
    new_centers_ref[...] = centers + delta
    new_sigmas_ref[...] = jnp.sqrt((heights * sigmas * sigmas + spread) / new_heights - delta * delta)

    def wait_sends(step, carry):
        copy_a(peer(step), me).wait_send()
        copy_b(peer(step), me).wait_send()
        return carry

    lax.fori_loop(1, kern_count, wait_sends, 0)
    for step in range(1, walk_count):
        def wait_send_c(index, carry):
            copy_c(step, index, my_chunk, walk).wait_send()
            return carry

        lax.fori_loop(0, chunks, wait_send_c, 0)
        for copy in copy_w(step, walk):
            copy.wait_send()


def write_kernel(*refs):
    count = (len(refs) - 1) // 2
    copies = [pltpu.make_async_copy(refs[i], refs[count + i], refs[-1].at[i]) for i in range(count)]
    for copy in copies:
        copy.start()
    for copy in copies:
        copy.wait()


def per_device(walkers, centers, sigmas, heights, kernel_live, merge_target, new_sigma, norm_old):
    dims, walk_len = walkers.shape
    shard_len = centers.shape[1]
    kern_count = lax.axis_size("kern")
    walk_count = lax.axis_size("walk")
    chunks = walk_len // LANES
    groups = kern_count // chunks
    per = dims // groups
    capacity = 2 * walk_len // kern_count
    height_row = heights.reshape(1, shard_len)

    dma = pltpu.SemaphoreType.DMA
    shapes = [(1, walk_len), (dims, walk_len), (1, shard_len), (dims, shard_len), (dims, shard_len), (1, 1)]
    results = pl.pallas_call(
        functools.partial(sums_kernel, kern_count, walk_count, groups, capacity),
        out_shape=[pltpu.VMEM(shape, F32) for shape in shapes],
        in_specs=[HBM] * 8,
        scratch_shapes=[
            pltpu.VMEM((dims, walk_len), F32),
            pltpu.VMEM((1, walk_len), jnp.int32),
            pltpu.VMEM((dims, shard_len), F32),
            pltpu.VMEM((dims, shard_len), F32),
            pltpu.VMEM((1, shard_len), F32),
            pltpu.SMEM((1,), jnp.int32),
            pltpu.SMEM((1,), F32),
            pltpu.VMEM((1, dims), F32),
            dma((8,)),
            pltpu.VMEM((walk_len // (2 * LANES), LANES, 2 * LANES), BF16),
            pltpu.VMEM((shard_len, LANES), BF16),
            pltpu.VMEM((6 * dims + 16, shard_len), BF16),
            pltpu.VMEM((kern_count, 2 * per + 2, LANES), F32),
            pltpu.VMEM((kern_count, per, LANES), F32),
            pltpu.VMEM((kern_count, 2 * per + 2, LANES), F32),
            pltpu.VMEM((per + 1, LANES), F32),
            pltpu.VMEM((kern_count, per + 1, LANES), F32),
            pltpu.VMEM((walk_count, chunks, per + 1, LANES), F32),
            pltpu.VMEM((walk_count, dims, walk_len), F32),
            pltpu.VMEM((walk_count, 1, walk_len), jnp.int32),
            pltpu.VMEM((walk_count, capacity, walk_len), BF16),
            pltpu.VMEM((walk_count, shard_len, capacity), BF16),
            dma((kern_count,)), dma((kern_count,)),
            dma((kern_count,)), dma((kern_count,)),
            dma((walk_count, chunks)), dma((walk_count, chunks)),
            dma((walk_count,)), dma((walk_count,)),
            dma((walk_count,)), dma((walk_count,)),
        ],
        compiler_params=pltpu.CompilerParams(collective_id=0, has_side_effects=True, vmem_limit_bytes=LIMIT),
        name="sums",
    )(*[
        pltpu.with_memory_space_constraint(x, pltpu.HBM)
        for x in (walkers, merge_target.reshape(1, walk_len), centers, sigmas, height_row)
    ], kernel_live, norm_old, pltpu.with_memory_space_constraint(new_sigma.reshape(1, dims), pltpu.HBM))

    bias, force, new_heights, new_centers, new_sigmas, log_norm = pl.pallas_call(
        write_kernel,
        out_shape=[jax.ShapeDtypeStruct(shape, F32) for shape in shapes],
        in_specs=[VMEM] * 6,
        out_specs=[HBM] * 6,
        scratch_shapes=[dma((6,))],
        compiler_params=pltpu.CompilerParams(vmem_limit_bytes=LIMIT),
        name="write",
    )(*results)
    return (bias.reshape(walk_len), force, new_heights.reshape(shard_len), new_centers, new_sigmas, log_norm.reshape(1))


def solution(mesh):
    in_specs = (
        P(None, "walk"),
        P(None, "kern"),
        P(None, "kern"),
        P("kern"),
        P("kern"),
        P("walk"),
        P(),
        P(),
    )
    out_specs = (P("walk"), P(None, "walk"), P("kern"), P(None, "kern"), P(None, "kern"), P())
    return jax.shard_map(
        per_device, mesh=mesh, in_specs=in_specs, out_specs=out_specs, check_vma=False
    )
```

```python
import functools
import math

import jax
import jax.numpy as jnp
from jax import lax
from jax.experimental import pallas as pl
from jax.experimental.pallas import tpu as pltpu
from jax.sharding import PartitionSpec as P

PREFACTOR = 0.9
EPSILON = 0.01
RATE = 0.25
LANES = 128
LOG2E = math.log2(math.e)
MESH = pl.DeviceIdType.MESH
F32 = jnp.float32
BF16 = jnp.bfloat16
VMEM = pl.BlockSpec(memory_space=pltpu.VMEM)
HBM = pl.BlockSpec(memory_space=pltpu.HBM)
LIMIT = 24 << 20


def split(x):
    high = x.astype(BF16).astype(F32)
    rest = x - high
    middle = rest.astype(BF16).astype(F32)
    low = (rest - middle).astype(BF16).astype(F32)
    return high, middle, low


def row_of(parts, width):
    row = lax.broadcasted_iota(jnp.int32, (8, width), 0)
    block = jnp.zeros((8, width), F32)
    for index, part in enumerate(parts):
        block = jnp.where(row == index, part, block)
    return block


def sums_kernel(kern_count, walk_count, owners, capacity,
                walkers_hbm, target_hbm, centers_hbm, sigmas_hbm, heights_hbm, live_hbm, norm_hbm, new_sigma_hbm,
                bias_ref, force_ref, new_heights_ref, new_centers_ref, new_sigmas_ref,
                walkers_ref, target_ref, centers_ref, sigmas_ref, heights_ref, live_ref, norm_ref, new_sigma_ref, load_sem,
                walker_feat, kernel_feat, kernel_mom, sums, got, early, early_got, early_far, direct, direct_far,
                mine, shared, far, far_walkers, far_targets, table, placing, spare,
                sent, recv_a, recv_d, recv_e, recv_b, recv_w):
    def load(source, target, index):
        return pltpu.make_async_copy(source, target, load_sem.at[index])

    wide = [
        load(walkers_hbm, walkers_ref, 0),
        load(centers_hbm, centers_ref, 0),
        load(sigmas_hbm, sigmas_ref, 0),
        load(heights_hbm, heights_ref, 0),
        load(target_hbm, target_ref, 0),
    ]
    narrow = [load(live_hbm, live_ref, 1), load(norm_hbm, norm_ref, 2), load(new_sigma_hbm, new_sigma_ref, 3)]
    for copy in wide + narrow:
        copy.start()
    dims, walk_len = walkers_ref.shape
    shard_len = centers_ref.shape[1]
    late = kern_count - owners
    rows = dims + 2
    me = lax.axis_index("kern")
    walk = lax.axis_index("walk")
    flat = me * walk_count + walk
    total_count = kern_count * walk_count

    others = walk_count - 1
    load_rows = (dims * (walk_len + 2 * shard_len) + shard_len + walk_len) // LANES
    walker_rows = others * (dims + 1) * walk_len // LANES

    def other(step):
        return lax.rem(walk + step, walk_count)

    def bulk(count, sem):
        view = spare.at[pl.ds(0, count)]
        return pltpu.make_async_remote_copy(
            src_ref=view, dst_ref=view, send_sem=sent, recv_sem=sem, device_id=(me, walk), device_id_type=MESH
        )

    barrier = pltpu.get_barrier_semaphore()

    def greet(step, carry):
        peer = lax.rem(flat + step, total_count)
        pl.semaphore_signal(
            barrier, inc=1, device_id=(peer // walk_count, lax.rem(peer, walk_count)), device_id_type=MESH
        )
        return carry

    lax.fori_loop(1, total_count, greet, 0)

    load(spare.at[pl.ds(0, load_rows)], spare.at[pl.ds(0, load_rows)], 0).wait()
    for copy in narrow:
        copy.wait()
    norm = norm_ref[0]
    walkers = walkers_ref[...]
    sq_h, sq_m, sq_l = split(walkers * walkers)
    wk_h, wk_m, wk_l = split(walkers)
    h, m, l = [sq_h, wk_h], [sq_m, wk_m], [sq_l, wk_l]
    one = jnp.ones((1, walk_len), F32)
    pad = jnp.zeros((LANES - 12 * dims - 8, walk_len), F32)
    stacked = jnp.concatenate(h + m + h + m + l + h + [row_of([one] * 3, walk_len), pad], 0)
    stacked = stacked.astype(BF16)
    width = 2 * LANES
    quarters = walk_len // width
    for quarter in range(quarters):
        walker_feat[quarter] = stacked[:, quarter * width : (quarter + 1) * width]

    centers = centers_ref[...]
    sigmas = sigmas_ref[...]
    inverse_var = 1.0 / (sigmas * sigmas)
    scaled = centers * inverse_var
    constant = jnp.log(heights_ref[...]) - 0.5 * jnp.sum(centers * scaled, 0, keepdims=True)
    k_sq = split((-0.5 * LOG2E) * inverse_var)
    k_lin = split(LOG2E * scaled)
    con = row_of(split(LOG2E * constant), shard_len)
    h, m, l = [[k_sq[i], k_lin[i]] for i in range(3)]
    pad = jnp.zeros((LANES - 12 * dims - 8, shard_len), F32)
    kernel_feat[...] = jnp.concatenate(h + h + m + m + h + l + [con, pad], 0).T.astype(BF16)

    live = live_ref[0]
    alive = (lax.broadcasted_iota(jnp.int32, (8, shard_len), 1) < live).astype(F32)
    mom_a = split(inverse_var * alive)
    mom_c = split(scaled * alive)
    pad = jnp.zeros((8, shard_len), F32)
    mom_rows = [mom_a[0], mom_c[0], mom_a[1], mom_c[1], mom_a[2], mom_c[2], row_of([alive], shard_len), pad]
    kernel_mom[...] = jnp.concatenate(mom_rows, 0).astype(BF16)

    live_row = jnp.full((1, LANES), live, jnp.int32).astype(F32)
    block = min(512, shard_len)

    def copy_a(owner, source):
        return pltpu.make_async_remote_copy(
            src_ref=sums.at[owner], dst_ref=got.at[source],
            send_sem=sent, recv_sem=recv_a.at[jnp.where(me < owners, 0, 1)],
            device_id=(owner, walk), device_id_type=MESH,
        )

    def copy_d(quarter, source):
        part = pl.ds(quarter * 2, 2)
        return pltpu.make_async_remote_copy(
            src_ref=sums.at[part], dst_ref=direct.at[source, part],
            send_sem=sent, recv_sem=recv_d.at[min(quarter, 1)],
            device_id=(0, walk), device_id_type=MESH,
        )

    def copy_g(step, quarter, source, origin):
        part = pl.ds(quarter * 2, 2)
        return pltpu.make_async_remote_copy(
            src_ref=sums.at[part, pl.ds(dims, 1)], dst_ref=direct_far.at[origin, source, part],
            send_sem=sent, recv_sem=recv_d.at[min(quarter, 1)],
            device_id=(0, other(step)), device_id_type=MESH,
        )

    def copy_e(source):
        return pltpu.make_async_remote_copy(
            src_ref=early, dst_ref=early_got.at[source],
            send_sem=sent, recv_sem=recv_e,
            device_id=(0, walk), device_id_type=MESH,
        )

    def copy_h(step, source, origin):
        return pltpu.make_async_remote_copy(
            src_ref=early.at[pl.ds(dims, 1)], dst_ref=early_far.at[origin, source],
            send_sem=sent, recv_sem=recv_e,
            device_id=(0, other(step)), device_id_type=MESH,
        )

    def copy_b(target, source):
        return pltpu.make_async_remote_copy(
            src_ref=mine, dst_ref=shared.at[source],
            send_sem=sent, recv_sem=recv_b,
            device_id=(target, walk), device_id_type=MESH,
        )

    def copy_c(step, target, source, origin):
        return pltpu.make_async_remote_copy(
            src_ref=mine.at[pl.ds(dims, 1)], dst_ref=far.at[origin, source],
            send_sem=sent, recv_sem=recv_b,
            device_id=(target, other(step)), device_id_type=MESH,
        )

    def copy_w(step, source):
        return (
            pltpu.make_async_remote_copy(
                src_ref=walkers_ref, dst_ref=far_walkers.at[source],
                send_sem=sent, recv_sem=recv_w,
                device_id=(me, other(step)), device_id_type=MESH,
            ),
            pltpu.make_async_remote_copy(
                src_ref=target_ref, dst_ref=far_targets.at[source],
                send_sem=sent, recv_sem=recv_w,
                device_id=(me, other(step)), device_id_type=MESH,
            ),
        )

    def compute(quarter):
        feat = walker_feat[quarter]
        moments = None
        for index in range(shard_len // block):
            part = slice(index * block, (index + 1) * block)
            e = jnp.exp2(jnp.dot(kernel_feat[part, :], feat, preferred_element_type=F32))
            high = e.astype(BF16)
            low = (e - high.astype(F32)).astype(BF16)
            moms = kernel_mom[:, part]
            add = jnp.dot(moms, high, preferred_element_type=F32) + jnp.dot(
                moms, low, preferred_element_type=F32
            )
            moments = add if moments is None else moments + add
        a_sum = moments[0:dims] + moments[2 * dims : 3 * dims] + moments[4 * dims : 5 * dims]
        c_sum = moments[dims : 2 * dims] + moments[3 * dims : 4 * dims] + moments[5 * dims : 6 * dims]
        density = moments[6 * dims : 6 * dims + 1]
        grad = c_sum - walkers_ref[:, quarter * width : (quarter + 1) * width] * a_sum
        for chunk in range(2):
            part = slice(chunk * LANES, (chunk + 1) * LANES)
            sums[quarter * 2 + chunk, 0:dims, :] = grad[:, part]
            sums[quarter * 2 + chunk, dims : dims + 1, :] = density[:, part]
            sums[quarter * 2 + chunk, dims + 1 : dims + 2, :] = live_row

    def sends_a(owner):
        return (me != owner) & (me < owners) if owner == 0 else me != owner

    def send(quarter):
        @pl.when(me >= owners)
        def _():
            copy_d(quarter, me - owners).start()
            for step in range(1, walk_count):
                copy_g(step, quarter, me - owners, walk).start()

        for owner in (2 * quarter, 2 * quarter + 1):
            @pl.when(sends_a(owner))
            def _():
                copy_a(owner, me).start()

    for quarter in range(quarters):
        compute(quarter)
        if quarter == 1:
            pl.semaphore_wait(barrier, total_count - 1)
            send(0)
            for step in range(1, walk_count):
                for copy in copy_w(step, walk):
                    copy.start()
        if quarter >= 1:
            send(quarter)

    far_walkers[walk] = walkers
    far_targets[walk] = target_ref[...]
    bulk(walker_rows, recv_w).wait_recv()
    targets = [far_targets[index] for index in range(walk_count)]
    if walk_count % 8:
        targets.append(jnp.full((8 - walk_count % 8, walk_len), -1, jnp.int32))
    local = jnp.concatenate(targets, 0) - me * shard_len
    owned = (local >= 0) & (local < shard_len)
    before = lax.broadcasted_iota(jnp.int32, (walk_len, walk_len), 0) < lax.broadcasted_iota(
        jnp.int32, (walk_len, walk_len), 1
    )
    place = jnp.dot(
        jnp.where(owned, 1.0, 0.0).astype(BF16),
        jnp.where(before, 1.0, 0.0).astype(BF16),
        preferred_element_type=F32,
    )
    place = jnp.where(owned, place, -1.0)
    slot = jnp.where(owned, (local + 1).astype(F32), 0.0)
    want = lax.broadcasted_iota(jnp.int32, (capacity, walk_len), 0).astype(F32)

    def pack(feat, index):
        return lax.dot_general(
            feat.astype(BF16), table[index], (((1,), (1,)), ((), ())), preferred_element_type=F32
        )

    slots = lax.broadcasted_iota(jnp.int32, (shard_len, capacity), 0).astype(F32)
    packed_walkers = []
    for index in range(walk_count):
        table[index] = jnp.where(want == place[index : index + 1], 1.0, 0.0).astype(BF16)
        high, middle, low = split(far_walkers[index])
        slot_rows = row_of(split(slot[index : index + 1]), walk_len)
        packed = pack(jnp.concatenate([high, middle, low, slot_rows], 0), index)
        packed_walkers.append(packed[0:dims] + (packed[dims : 2 * dims] + packed[2 * dims : 3 * dims]))
        at = 3 * dims
        packed_slot = packed[at : at + 1] + packed[at + 1 : at + 2] + packed[at + 2 : at + 3] - 1.0
        placing[index] = jnp.where(slots == packed_slot, 1.0, 0.0).astype(BF16)

    def finish(total):
        live_total = total[dims + 1 : dims + 2]
        density = total[dims : dims + 1] / live_total
        ratio = density / norm + EPSILON
        return density, -PREFACTOR * (total[0:dims] / live_total) / (norm * ratio)

    def publish(total):
        density, force = finish(total)
        mine[0:dims, :] = force
        mine[dims : dims + 1, :] = density

        def start_b(target, carry):
            @pl.when(target != me)
            def _():
                copy_b(target, me).start()

            for step in range(1, walk_count):
                copy_c(step, target, me, walk).start()
            return carry

        lax.fori_loop(1, kern_count, start_b, 0)
        shared[me, 0:dims, :] = force
        shared[me, dims : dims + 1, :] = density

    @pl.when(me < owners)
    def _():
        got[me] = sums[me]

        bulk((owners - 1) * rows, recv_a.at[0]).wait_recv()
        total = got[0]
        for source in range(1, owners):
            total = total + got[source]
        early[...] = total
        for step in range(1, walk_count):
            copy_h(step, me, walk).start()

        @pl.when(me > 0)
        def _():
            copy_e(me).start()

            bulk(late * rows, recv_a.at[1]).wait_recv()
            whole = total
            for source in range(owners, kern_count):
                whole = whole + got[source]
            publish(whole)

        @pl.when(me == 0)
        def _():
            def late_sum(chunk, whole):
                for source in range(late):
                    whole = whole + direct[source, chunk]
                return whole

            bulk(late * 2 * (rows + others), recv_d.at[0]).wait_recv()
            publish(late_sum(0, total))

            bulk((owners - 1) * rows + others * owners, recv_e).wait_recv()
            bulk(late * (owners - 2) * (rows + others), recv_d.at[1]).wait_recv()
            for chunk in range(1, owners):
                density, force = finish(late_sum(chunk, early_got[chunk]))
                shared[chunk, 0:dims, :] = force
                shared[chunk, dims : dims + 1, :] = density
            live_total = late_sum(0, total)[dims + 1 : dims + 2]
            for step in range(1, walk_count):
                origin = other(step)
                for chunk in range(owners):
                    whole = early_far[origin, chunk]
                    for source in range(late):
                        whole = whole + direct_far[origin, source, chunk]
                    far[origin, chunk] = whole / live_total

    @pl.when((me > 0) & (me < owners))
    def _():
        bulk((owners - 1) * (dims + 1) + others * owners, recv_b).wait_recv()

    @pl.when(me >= owners)
    def _():
        bulk(owners * (dims + 1) + others * owners, recv_b).wait_recv()

    def biased(density):
        return PREFACTOR * jnp.log(density / norm + EPSILON)

    for chunk in range(owners):
        part = slice(chunk * LANES, (chunk + 1) * LANES)
        density = shared[chunk, dims : dims + 1, :]
        far[walk, chunk] = density
        bias_ref[:, part] = biased(density)
        force_ref[:, part] = shared[chunk, 0:dims, :]
    density_sum = jnp.zeros((1, 1), F32)
    merged = None
    for index in range(walk_count):
        whole = jnp.concatenate([far[index, chunk] for chunk in range(owners)], 1)
        density_sum = density_sum + jnp.sum(whole, 1, keepdims=True)
        packed = pack(row_of(split(whole), walk_len), index)
        weight = jnp.exp(biased(packed[0:1] + packed[1:2] + packed[2:3]))
        lin = split(weight * packed_walkers[index])
        sq = split(weight * (packed_walkers[index] * packed_walkers[index]))
        last = row_of(split(weight), capacity)
        pad = jnp.zeros((8, capacity), F32)
        feat = jnp.concatenate([lin[0], sq[0], lin[1], sq[1], lin[2], sq[2], last, pad], 0).astype(BF16)
        add = lax.dot_general(feat, placing[index], (((1,), (1,)), ((), ())), preferred_element_type=F32)
        merged = add if merged is None else merged + add
    log_norm = jnp.log((1.0 - RATE) * norm + RATE * density_sum / (walk_len * walk_count))
    bias_ref[:, walk_len : walk_len + LANES] = jnp.broadcast_to(log_norm, (1, LANES))

    first = merged[0:dims] + (merged[2 * dims : 3 * dims] + merged[4 * dims : 5 * dims])
    second = merged[dims : 2 * dims] + (merged[3 * dims : 4 * dims] + merged[5 * dims : 6 * dims])
    at = 6 * dims
    gain = merged[at : at + 1] + (merged[at + 1 : at + 2] + merged[at + 2 : at + 3])
    row = lax.broadcasted_iota(jnp.int32, (dims, dims), 0)
    column = lax.broadcasted_iota(jnp.int32, (dims, dims), 1)
    new_sigma = jnp.sum(jnp.where(row == column, new_sigma_ref[...], 0.0), 1, keepdims=True)
    centers = centers_ref[...]
    sigmas = sigmas_ref[...]
    heights = heights_ref[...]
    shift = first - centers * gain
    spread = second - 2.0 * centers * first + centers * centers * gain + new_sigma * new_sigma * gain
    new_heights = heights + gain
    delta = shift / new_heights
    new_heights_ref[...] = new_heights
    new_centers_ref[...] = centers + delta
    new_sigmas_ref[...] = jnp.sqrt((heights * sigmas * sigmas + spread) / new_heights - delta * delta)

    always = walker_rows + (owners - 1) * rows
    answers = others * (kern_count - 1) + (kern_count - 2) * (dims + 1) + others

    @pl.when(me >= owners)
    def _():
        bulk(always + owners * (rows + others), sent).wait_send()

    @pl.when((me > 0) & (me < owners))
    def _():
        bulk(always + answers + rows, sent).wait_send()

    @pl.when(me == 0)
    def _():
        bulk(always + answers + dims + 1, sent).wait_send()


def write_kernel(bias_ref, force_ref, new_heights_ref, new_centers_ref, new_sigmas_ref,
                 bias_hbm, force_hbm, new_heights_hbm, new_centers_hbm, new_sigmas_hbm, log_norm_hbm, log_norm_ref, sem):
    walk_len = bias_hbm.shape[1]
    log_norm_ref[...] = bias_ref[:, walk_len : walk_len + 1]
    pairs = [
        (new_centers_ref, new_centers_hbm),
        (new_sigmas_ref, new_sigmas_hbm),
        (force_ref, force_hbm),
        (new_heights_ref, new_heights_hbm),
        (bias_ref.at[:, pl.ds(0, walk_len)], bias_hbm),
        (log_norm_ref, log_norm_hbm),
    ]
    copies = [pltpu.make_async_copy(source, target, sem.at[index]) for index, (source, target) in enumerate(pairs)]
    for copy in copies:
        copy.start()
    for copy in copies:
        copy.wait()


def per_device(walkers, centers, sigmas, heights, kernel_live, merge_target, new_sigma, norm_old):
    dims, walk_len = walkers.shape
    shard_len = centers.shape[1]
    kern_count = lax.axis_size("kern")
    walk_count = lax.axis_size("walk")
    owners = walk_len // LANES
    late = kern_count - owners
    quarters = owners // 2
    rows = dims + 2
    capacity = 2 * walk_len // kern_count
    height_row = heights.reshape(1, shard_len)
    load_rows = (dims * (walk_len + 2 * shard_len) + shard_len + walk_len) // LANES
    walker_rows = walk_count * (dims + 1) * walk_len // LANES
    answer_rows = walk_count * kern_count + kern_count * rows
    spare_rows = load_rows + walker_rows + answer_rows + kern_count * owners * (rows + walk_count)

    dma = pltpu.SemaphoreType.DMA
    shapes = [(1, walk_len), (dims, walk_len), (1, shard_len), (dims, shard_len), (dims, shard_len), (1, 1)]
    results = pl.pallas_call(
        functools.partial(sums_kernel, kern_count, walk_count, owners, capacity),
        out_shape=[pltpu.VMEM(shape, F32) for shape in [(1, walk_len + LANES)] + shapes[1:5]],
        in_specs=[HBM] * 8,
        scratch_shapes=[
            pltpu.VMEM((dims, walk_len), F32),
            pltpu.VMEM((1, walk_len), jnp.int32),
            pltpu.VMEM((dims, shard_len), F32),
            pltpu.VMEM((dims, shard_len), F32),
            pltpu.VMEM((1, shard_len), F32),
            pltpu.SMEM((1,), jnp.int32),
            pltpu.SMEM((1,), F32),
            pltpu.VMEM((1, dims), F32),
            dma((4,)),
            pltpu.VMEM((walk_len // (2 * LANES), LANES, 2 * LANES), BF16),
            pltpu.VMEM((shard_len, LANES), BF16),
            pltpu.VMEM((6 * dims + 16, shard_len), BF16),
            pltpu.VMEM((owners, rows, LANES), F32),
            pltpu.VMEM((kern_count, rows, LANES), F32),
            pltpu.VMEM((rows, LANES), F32),
            pltpu.VMEM((owners, rows, LANES), F32),
            pltpu.VMEM((walk_count, owners, 1, LANES), F32),
            pltpu.VMEM((late, owners, rows, LANES), F32),
            pltpu.VMEM((walk_count, late, owners, 1, LANES), F32),
            pltpu.VMEM((dims + 1, LANES), F32),
            pltpu.VMEM((owners, dims + 1, LANES), F32),
            pltpu.VMEM((walk_count, owners, 1, LANES), F32),
            pltpu.VMEM((walk_count, dims, walk_len), F32),
            pltpu.VMEM((walk_count, 1, walk_len), jnp.int32),
            pltpu.VMEM((walk_count, capacity, walk_len), BF16),
            pltpu.VMEM((walk_count, shard_len, capacity), BF16),
            pltpu.VMEM((spare_rows, LANES), F32),
            dma, dma((2,)), dma((2,)), dma, dma, dma,
        ],
        compiler_params=pltpu.CompilerParams(collective_id=0, has_side_effects=True, vmem_limit_bytes=LIMIT),
        name="sums",
    )(*[
        pltpu.with_memory_space_constraint(x, pltpu.HBM)
        for x in (walkers, merge_target.reshape(1, walk_len), centers, sigmas, height_row)
    ], kernel_live, norm_old, pltpu.with_memory_space_constraint(new_sigma.reshape(1, dims), pltpu.HBM))

    bias, force, new_heights, new_centers, new_sigmas, log_norm = pl.pallas_call(
        write_kernel,
        out_shape=[jax.ShapeDtypeStruct(shape, F32) for shape in shapes],
        in_specs=[VMEM] * 5,
        out_specs=[HBM] * 6,
        scratch_shapes=[pltpu.VMEM((1, 1), F32), dma((6,))],
        compiler_params=pltpu.CompilerParams(vmem_limit_bytes=LIMIT),
        name="write",
    )(*results)
    return (bias.reshape(walk_len), force, new_heights.reshape(shard_len), new_centers, new_sigmas, log_norm.reshape(1))


def solution(mesh):
    in_specs = (
        P(None, "walk"),
        P(None, "kern"),
        P(None, "kern"),
        P("kern"),
        P("kern"),
        P("walk"),
        P(),
        P(),
    )
    out_specs = (P("walk"), P(None, "walk"), P("kern"), P(None, "kern"), P(None, "kern"), P())
    return jax.shard_map(
        per_device, mesh=mesh, in_specs=in_specs, out_specs=out_specs, check_vma=False
    )
```

```python
import functools
import math

import jax
import jax.numpy as jnp
from jax import lax
from jax.experimental import pallas as pl
from jax.experimental.pallas import tpu as pltpu
from jax.sharding import PartitionSpec as P

PREFACTOR = 0.9
EPSILON = 0.01
RATE = 0.25
LANES = 128
LOG2E = math.log2(math.e)
MESH = pl.DeviceIdType.MESH
F32 = jnp.float32
BF16 = jnp.bfloat16
VMEM = pl.BlockSpec(memory_space=pltpu.VMEM)
HBM = pl.BlockSpec(memory_space=pltpu.HBM)
LIMIT = 24 << 20


def split(x):
    high = x.astype(BF16).astype(F32)
    rest = x - high
    middle = rest.astype(BF16).astype(F32)
    low = (rest - middle).astype(BF16).astype(F32)
    return high, middle, low


def row_of(parts, width):
    row = lax.broadcasted_iota(jnp.int32, (8, width), 0)
    block = jnp.zeros((8, width), F32)
    for index, part in enumerate(parts):
        block = jnp.where(row == index, part, block)
    return block


def sums_kernel(kern_count, walk_count, owners, capacity,
                walkers_hbm, target_hbm, centers_hbm, sigmas_hbm, heights_hbm, live_hbm, norm_hbm, new_sigma_hbm,
                bias_ref, force_ref, new_heights_ref, new_centers_ref, new_sigmas_ref,
                walkers_ref, target_ref, centers_ref, sigmas_ref, heights_ref, live_ref, norm_ref, new_sigma_ref, load_sem,
                walker_feat, kernel_feat, kernel_mom, sums, got, early, early_got, early_far, direct, direct_far,
                mine, shared, far, far_walkers, far_targets, table, placing, spare,
                ready, sent, recv_a, recv_d, recv_e, recv_b, recv_w):
    def load(source, target, index):
        return pltpu.make_async_copy(source, target, load_sem.at[index])

    wide = [
        load(walkers_hbm, walkers_ref, 0),
        load(centers_hbm, centers_ref, 0),
        load(sigmas_hbm, sigmas_ref, 0),
        load(heights_hbm, heights_ref, 0),
        load(target_hbm, target_ref, 0),
    ]
    narrow = [load(live_hbm, live_ref, 1), load(norm_hbm, norm_ref, 2), load(new_sigma_hbm, new_sigma_ref, 3)]
    for copy in wide + narrow:
        copy.start()
    dims, walk_len = walkers_ref.shape
    shard_len = centers_ref.shape[1]
    late = kern_count - owners
    rows = dims + 2
    me = lax.axis_index("kern")
    walk = lax.axis_index("walk")
    flat = me * walk_count + walk
    total_count = kern_count * walk_count

    others = walk_count - 1
    load_rows = (dims * (walk_len + 2 * shard_len) + shard_len + walk_len) // LANES
    walker_rows = others * (dims + 1) * walk_len // LANES

    def other(step):
        return lax.rem(walk + step, walk_count)

    def bulk(count, sem):
        view = spare.at[pl.ds(0, count)]
        return pltpu.make_async_remote_copy(
            src_ref=view, dst_ref=view, send_sem=sent, recv_sem=sem, device_id=(me, walk), device_id_type=MESH
        )

    barrier = pltpu.get_barrier_semaphore()

    def greet(peer):
        pl.semaphore_signal(
            barrier, inc=1, device_id=(peer // walk_count, lax.rem(peer, walk_count)), device_id_type=MESH
        )

    @pl.when(me < owners)
    def _():
        def greet_all(step, carry):
            greet(lax.rem(flat + step, total_count))
            return carry

        lax.fori_loop(1, total_count, greet_all, 0)

    @pl.when(me >= owners)
    def _():
        for step in range(1, walk_count):
            greet(me * walk_count + other(step))

    load(spare.at[pl.ds(0, load_rows)], spare.at[pl.ds(0, load_rows)], 0).wait()
    for copy in narrow:
        copy.wait()
    norm = norm_ref[0]
    walkers = walkers_ref[...]
    sq_h, sq_m, sq_l = split(walkers * walkers)
    wk_h, wk_m, wk_l = split(walkers)
    h, m, l = [sq_h, wk_h], [sq_m, wk_m], [sq_l, wk_l]
    one = jnp.ones((1, walk_len), F32)
    pad = jnp.zeros((LANES - 12 * dims - 8, walk_len), F32)
    stacked = jnp.concatenate(h + m + h + m + l + h + [row_of([one] * 3, walk_len), pad], 0)
    stacked = stacked.astype(BF16)
    width = 2 * LANES
    quarters = walk_len // width
    for quarter in range(quarters):
        walker_feat[quarter] = stacked[:, quarter * width : (quarter + 1) * width]

    centers = centers_ref[...]
    sigmas = sigmas_ref[...]
    inverse_var = 1.0 / (sigmas * sigmas)
    scaled = centers * inverse_var
    constant = jnp.log(heights_ref[...]) - 0.5 * jnp.sum(centers * scaled, 0, keepdims=True)
    k_sq = split((-0.5 * LOG2E) * inverse_var)
    k_lin = split(LOG2E * scaled)
    con = row_of(split(LOG2E * constant), shard_len)
    h, m, l = [[k_sq[i], k_lin[i]] for i in range(3)]
    pad = jnp.zeros((LANES - 12 * dims - 8, shard_len), F32)
    kernel_feat[...] = jnp.concatenate(h + h + m + m + h + l + [con, pad], 0).T.astype(BF16)

    live = live_ref[0]
    alive = (lax.broadcasted_iota(jnp.int32, (8, shard_len), 1) < live).astype(F32)
    mom_a = split(inverse_var * alive)
    mom_c = split(scaled * alive)
    pad = jnp.zeros((8, shard_len), F32)
    mom_rows = [mom_a[0], mom_c[0], mom_a[1], mom_c[1], mom_a[2], mom_c[2], row_of([alive], shard_len), pad]
    kernel_mom[...] = jnp.concatenate(mom_rows, 0).astype(BF16)

    live_row = jnp.full((1, LANES), live, jnp.int32).astype(F32)
    block = min(512, shard_len)

    def copy_a(owner, source):
        return pltpu.make_async_remote_copy(
            src_ref=sums.at[owner], dst_ref=got.at[source],
            send_sem=sent, recv_sem=recv_a.at[jnp.where(me < owners, 0, 1)],
            device_id=(owner, walk), device_id_type=MESH,
        )

    def copy_d(quarter, source):
        part = pl.ds(quarter * 2, 2)
        return pltpu.make_async_remote_copy(
            src_ref=sums.at[part], dst_ref=direct.at[source, part],
            send_sem=sent, recv_sem=recv_d.at[min(quarter, 1)],
            device_id=(0, walk), device_id_type=MESH,
        )

    def copy_g(step, quarter, source, origin):
        part = pl.ds(quarter * 2, 2)
        return pltpu.make_async_remote_copy(
            src_ref=sums.at[part, pl.ds(dims, 1)], dst_ref=direct_far.at[origin, source, part],
            send_sem=sent, recv_sem=recv_d.at[min(quarter, 1)],
            device_id=(0, other(step)), device_id_type=MESH,
        )

    def copy_e(source):
        return pltpu.make_async_remote_copy(
            src_ref=early, dst_ref=early_got.at[source],
            send_sem=sent, recv_sem=recv_e,
            device_id=(0, walk), device_id_type=MESH,
        )

    def copy_h(step, source, origin):
        return pltpu.make_async_remote_copy(
            src_ref=early.at[pl.ds(dims, 1)], dst_ref=early_far.at[origin, source],
            send_sem=sent, recv_sem=recv_e,
            device_id=(0, other(step)), device_id_type=MESH,
        )

    def copy_b(target, source):
        return pltpu.make_async_remote_copy(
            src_ref=mine, dst_ref=shared.at[source],
            send_sem=sent, recv_sem=recv_b,
            device_id=(target, walk), device_id_type=MESH,
        )

    def copy_c(step, target, source, origin):
        return pltpu.make_async_remote_copy(
            src_ref=mine.at[pl.ds(dims, 1)], dst_ref=far.at[origin, source],
            send_sem=sent, recv_sem=recv_b,
            device_id=(target, other(step)), device_id_type=MESH,
        )

    def copy_w(step, source):
        return (
            pltpu.make_async_remote_copy(
                src_ref=walkers_ref, dst_ref=far_walkers.at[source],
                send_sem=sent, recv_sem=recv_w,
                device_id=(me, other(step)), device_id_type=MESH,
            ),
            pltpu.make_async_remote_copy(
                src_ref=target_ref, dst_ref=far_targets.at[source],
                send_sem=sent, recv_sem=recv_w,
                device_id=(me, other(step)), device_id_type=MESH,
            ),
        )

    def compute(quarter):
        feat = walker_feat[quarter]
        moments = None
        for index in range(shard_len // block):
            part = slice(index * block, (index + 1) * block)
            e = jnp.exp2(jnp.dot(kernel_feat[part, :], feat, preferred_element_type=F32))
            high = e.astype(BF16)
            low = (e - high.astype(F32)).astype(BF16)
            moms = kernel_mom[:, part]
            add = jnp.dot(moms, high, preferred_element_type=F32) + jnp.dot(
                moms, low, preferred_element_type=F32
            )
            moments = add if moments is None else moments + add
        a_sum = moments[0:dims] + moments[2 * dims : 3 * dims] + moments[4 * dims : 5 * dims]
        c_sum = moments[dims : 2 * dims] + moments[3 * dims : 4 * dims] + moments[5 * dims : 6 * dims]
        density = moments[6 * dims : 6 * dims + 1]
        grad = c_sum - walkers_ref[:, quarter * width : (quarter + 1) * width] * a_sum
        for chunk in range(2):
            part = slice(chunk * LANES, (chunk + 1) * LANES)
            sums[quarter * 2 + chunk, 0:dims, :] = grad[:, part]
            sums[quarter * 2 + chunk, dims : dims + 1, :] = density[:, part]
            sums[quarter * 2 + chunk, dims + 1 : dims + 2, :] = live_row

    def sends_a(owner):
        return (me != owner) & (me < owners) if owner == 0 else me != owner

    def send(quarter):
        @pl.when(me >= owners)
        def _():
            copy_d(quarter, me - owners).start()
            for step in range(1, walk_count):
                copy_g(step, quarter, me - owners, walk).start()

        for owner in (2 * quarter, 2 * quarter + 1):
            @pl.when(sends_a(owner))
            def _():
                copy_a(owner, me).start()

    for quarter in range(quarters):
        compute(quarter)
        if quarter == 1:
            @pl.when(me < owners)
            def _():
                pl.semaphore_wait(barrier, owners * walk_count - 1)

            @pl.when(me >= owners)
            def _():
                pl.semaphore_wait(barrier, owners * walk_count + others)

                def tell(peer, carry):
                    pl.semaphore_signal(
                        ready, inc=1, device_id=(peer // walk_count, lax.rem(peer, walk_count)), device_id_type=MESH
                    )
                    return carry

                lax.fori_loop(0, owners * walk_count, tell, 0)

            send(0)
            for step in range(1, walk_count):
                for copy in copy_w(step, walk):
                    copy.start()
        if quarter >= 1:
            send(quarter)

    far_walkers[walk] = walkers
    far_targets[walk] = target_ref[...]
    bulk(walker_rows, recv_w).wait_recv()
    targets = [far_targets[index] for index in range(walk_count)]
    if walk_count % 8:
        targets.append(jnp.full((8 - walk_count % 8, walk_len), -1, jnp.int32))
    local = jnp.concatenate(targets, 0) - me * shard_len
    owned = (local >= 0) & (local < shard_len)
    before = lax.broadcasted_iota(jnp.int32, (walk_len, walk_len), 0) < lax.broadcasted_iota(
        jnp.int32, (walk_len, walk_len), 1
    )
    place = jnp.dot(
        jnp.where(owned, 1.0, 0.0).astype(BF16),
        jnp.where(before, 1.0, 0.0).astype(BF16),
        preferred_element_type=F32,
    )
    place = jnp.where(owned, place, -1.0)
    slot = jnp.where(owned, (local + 1).astype(F32), 0.0)
    want = lax.broadcasted_iota(jnp.int32, (capacity, walk_len), 0).astype(F32)

    def pack(feat, index):
        return lax.dot_general(
            feat.astype(BF16), table[index], (((1,), (1,)), ((), ())), preferred_element_type=F32
        )

    slots = lax.broadcasted_iota(jnp.int32, (shard_len, capacity), 0).astype(F32)
    packed_walkers = []
    for index in range(walk_count):
        table[index] = jnp.where(want == place[index : index + 1], 1.0, 0.0).astype(BF16)
        high, middle, low = split(far_walkers[index])
        slot_rows = row_of(split(slot[index : index + 1]), walk_len)
        packed = pack(jnp.concatenate([high, middle, low, slot_rows], 0), index)
        packed_walkers.append(packed[0:dims] + (packed[dims : 2 * dims] + packed[2 * dims : 3 * dims]))
        at = 3 * dims
        packed_slot = packed[at : at + 1] + packed[at + 1 : at + 2] + packed[at + 2 : at + 3] - 1.0
        placing[index] = jnp.where(slots == packed_slot, 1.0, 0.0).astype(BF16)

    def finish(total):
        live_total = total[dims + 1 : dims + 2]
        density = total[dims : dims + 1] / live_total
        ratio = density / norm + EPSILON
        return density, -PREFACTOR * (total[0:dims] / live_total) / (norm * ratio)

    def publish(total):
        pl.semaphore_wait(ready, late * walk_count)
        density, force = finish(total)
        mine[0:dims, :] = force
        mine[dims : dims + 1, :] = density

        def start_b(target, carry):
            @pl.when(target != me)
            def _():
                copy_b(target, me).start()

            for step in range(1, walk_count):
                copy_c(step, target, me, walk).start()
            return carry

        lax.fori_loop(1, kern_count, start_b, 0)
        shared[me, 0:dims, :] = force
        shared[me, dims : dims + 1, :] = density

    @pl.when(me < owners)
    def _():
        got[me] = sums[me]

        bulk((owners - 1) * rows, recv_a.at[0]).wait_recv()
        total = got[0]
        for source in range(1, owners):
            total = total + got[source]
        early[...] = total
        for step in range(1, walk_count):
            copy_h(step, me, walk).start()

        @pl.when(me > 0)
        def _():
            copy_e(me).start()

            bulk(late * rows, recv_a.at[1]).wait_recv()
            whole = total
            for source in range(owners, kern_count):
                whole = whole + got[source]
            publish(whole)

        @pl.when(me == 0)
        def _():
            def late_sum(chunk, whole):
                for source in range(late):
                    whole = whole + direct[source, chunk]
                return whole

            bulk(late * 2 * (rows + others), recv_d.at[0]).wait_recv()
            publish(late_sum(0, total))

            bulk((owners - 1) * rows + others * owners, recv_e).wait_recv()
            bulk(late * (owners - 2) * (rows + others), recv_d.at[1]).wait_recv()
            for chunk in range(1, owners):
                density, force = finish(late_sum(chunk, early_got[chunk]))
                shared[chunk, 0:dims, :] = force
                shared[chunk, dims : dims + 1, :] = density
            live_total = late_sum(0, total)[dims + 1 : dims + 2]
            for step in range(1, walk_count):
                origin = other(step)
                for chunk in range(owners):
                    whole = early_far[origin, chunk]
                    for source in range(late):
                        whole = whole + direct_far[origin, source, chunk]
                    far[origin, chunk] = whole / live_total

    @pl.when((me > 0) & (me < owners))
    def _():
        bulk((owners - 1) * (dims + 1) + others * owners, recv_b).wait_recv()

    @pl.when(me >= owners)
    def _():
        bulk(owners * (dims + 1) + others * owners, recv_b).wait_recv()

    def biased(density):
        return PREFACTOR * jnp.log(density / norm + EPSILON)

    for chunk in range(owners):
        part = slice(chunk * LANES, (chunk + 1) * LANES)
        density = shared[chunk, dims : dims + 1, :]
        far[walk, chunk] = density
        bias_ref[:, part] = biased(density)
        force_ref[:, part] = shared[chunk, 0:dims, :]
    density_sum = jnp.zeros((1, 1), F32)
    merged = None
    for index in range(walk_count):
        whole = jnp.concatenate([far[index, chunk] for chunk in range(owners)], 1)
        density_sum = density_sum + jnp.sum(whole, 1, keepdims=True)
        packed = pack(row_of(split(whole), walk_len), index)
        weight = jnp.exp(biased(packed[0:1] + packed[1:2] + packed[2:3]))
        lin = split(weight * packed_walkers[index])
        sq = split(weight * (packed_walkers[index] * packed_walkers[index]))
        last = row_of(split(weight), capacity)
        pad = jnp.zeros((8, capacity), F32)
        feat = jnp.concatenate([lin[0], sq[0], lin[1], sq[1], lin[2], sq[2], last, pad], 0).astype(BF16)
        add = lax.dot_general(feat, placing[index], (((1,), (1,)), ((), ())), preferred_element_type=F32)
        merged = add if merged is None else merged + add
    log_norm = jnp.log((1.0 - RATE) * norm + RATE * density_sum / (walk_len * walk_count))
    bias_ref[:, walk_len : walk_len + LANES] = jnp.broadcast_to(log_norm, (1, LANES))

    first = merged[0:dims] + (merged[2 * dims : 3 * dims] + merged[4 * dims : 5 * dims])
    second = merged[dims : 2 * dims] + (merged[3 * dims : 4 * dims] + merged[5 * dims : 6 * dims])
    at = 6 * dims
    gain = merged[at : at + 1] + (merged[at + 1 : at + 2] + merged[at + 2 : at + 3])
    row = lax.broadcasted_iota(jnp.int32, (dims, dims), 0)
    column = lax.broadcasted_iota(jnp.int32, (dims, dims), 1)
    new_sigma = jnp.sum(jnp.where(row == column, new_sigma_ref[...], 0.0), 1, keepdims=True)
    centers = centers_ref[...]
    sigmas = sigmas_ref[...]
    heights = heights_ref[...]
    shift = first - centers * gain
    spread = second - 2.0 * centers * first + centers * centers * gain + new_sigma * new_sigma * gain
    new_heights = heights + gain
    delta = shift / new_heights
    new_heights_ref[...] = new_heights
    new_centers_ref[...] = centers + delta
    new_sigmas_ref[...] = jnp.sqrt((heights * sigmas * sigmas + spread) / new_heights - delta * delta)

    always = walker_rows + (owners - 1) * rows
    answers = others * (kern_count - 1) + (kern_count - 2) * (dims + 1) + others

    @pl.when(me >= owners)
    def _():
        bulk(always + owners * (rows + others), sent).wait_send()

    @pl.when((me > 0) & (me < owners))
    def _():
        bulk(always + answers + rows, sent).wait_send()

    @pl.when(me == 0)
    def _():
        bulk(always + answers + dims + 1, sent).wait_send()


def write_kernel(bias_ref, force_ref, new_heights_ref, new_centers_ref, new_sigmas_ref,
                 bias_hbm, force_hbm, new_heights_hbm, new_centers_hbm, new_sigmas_hbm, log_norm_hbm, log_norm_ref, sem):
    walk_len = bias_hbm.shape[1]
    log_norm_ref[...] = bias_ref[:, walk_len : walk_len + 1]
    pairs = [
        (new_centers_ref, new_centers_hbm),
        (new_sigmas_ref, new_sigmas_hbm),
        (force_ref, force_hbm),
        (new_heights_ref, new_heights_hbm),
        (bias_ref.at[:, pl.ds(0, walk_len)], bias_hbm),
        (log_norm_ref, log_norm_hbm),
    ]
    copies = [pltpu.make_async_copy(source, target, sem.at[index]) for index, (source, target) in enumerate(pairs)]
    for copy in copies:
        copy.start()
    for copy in copies:
        copy.wait()


def per_device(walkers, centers, sigmas, heights, kernel_live, merge_target, new_sigma, norm_old):
    dims, walk_len = walkers.shape
    shard_len = centers.shape[1]
    kern_count = lax.axis_size("kern")
    walk_count = lax.axis_size("walk")
    owners = walk_len // LANES
    late = kern_count - owners
    quarters = owners // 2
    rows = dims + 2
    capacity = 2 * walk_len // kern_count
    height_row = heights.reshape(1, shard_len)
    load_rows = (dims * (walk_len + 2 * shard_len) + shard_len + walk_len) // LANES
    walker_rows = walk_count * (dims + 1) * walk_len // LANES
    answer_rows = walk_count * kern_count + kern_count * rows
    spare_rows = load_rows + walker_rows + answer_rows + kern_count * owners * (rows + walk_count)

    dma = pltpu.SemaphoreType.DMA
    shapes = [(1, walk_len), (dims, walk_len), (1, shard_len), (dims, shard_len), (dims, shard_len), (1, 1)]
    results = pl.pallas_call(
        functools.partial(sums_kernel, kern_count, walk_count, owners, capacity),
        out_shape=[pltpu.VMEM(shape, F32) for shape in [(1, walk_len + LANES)] + shapes[1:5]],
        in_specs=[HBM] * 8,
        scratch_shapes=[
            pltpu.VMEM((dims, walk_len), F32),
            pltpu.VMEM((1, walk_len), jnp.int32),
            pltpu.VMEM((dims, shard_len), F32),
            pltpu.VMEM((dims, shard_len), F32),
            pltpu.VMEM((1, shard_len), F32),
            pltpu.SMEM((1,), jnp.int32),
            pltpu.SMEM((1,), F32),
            pltpu.VMEM((1, dims), F32),
            dma((4,)),
            pltpu.VMEM((walk_len // (2 * LANES), LANES, 2 * LANES), BF16),
            pltpu.VMEM((shard_len, LANES), BF16),
            pltpu.VMEM((6 * dims + 16, shard_len), BF16),
            pltpu.VMEM((owners, rows, LANES), F32),
            pltpu.VMEM((kern_count, rows, LANES), F32),
            pltpu.VMEM((rows, LANES), F32),
            pltpu.VMEM((owners, rows, LANES), F32),
            pltpu.VMEM((walk_count, owners, 1, LANES), F32),
            pltpu.VMEM((late, owners, rows, LANES), F32),
            pltpu.VMEM((walk_count, late, owners, 1, LANES), F32),
            pltpu.VMEM((dims + 1, LANES), F32),
            pltpu.VMEM((owners, dims + 1, LANES), F32),
            pltpu.VMEM((walk_count, owners, 1, LANES), F32),
            pltpu.VMEM((walk_count, dims, walk_len), F32),
            pltpu.VMEM((walk_count, 1, walk_len), jnp.int32),
            pltpu.VMEM((walk_count, capacity, walk_len), BF16),
            pltpu.VMEM((walk_count, shard_len, capacity), BF16),
            pltpu.VMEM((spare_rows, LANES), F32),
            pltpu.SemaphoreType.REGULAR, dma, dma((2,)), dma((2,)), dma, dma, dma,
        ],
        compiler_params=pltpu.CompilerParams(collective_id=0, has_side_effects=True, vmem_limit_bytes=LIMIT),
        name="sums",
    )(*[
        pltpu.with_memory_space_constraint(x, pltpu.HBM)
        for x in (walkers, merge_target.reshape(1, walk_len), centers, sigmas, height_row)
    ], kernel_live, norm_old, pltpu.with_memory_space_constraint(new_sigma.reshape(1, dims), pltpu.HBM))

    bias, force, new_heights, new_centers, new_sigmas, log_norm = pl.pallas_call(
        write_kernel,
        out_shape=[jax.ShapeDtypeStruct(shape, F32) for shape in shapes],
        in_specs=[VMEM] * 5,
        out_specs=[HBM] * 6,
        scratch_shapes=[pltpu.VMEM((1, 1), F32), dma((6,))],
        compiler_params=pltpu.CompilerParams(vmem_limit_bytes=LIMIT),
        name="write",
    )(*results)
    return (bias.reshape(walk_len), force, new_heights.reshape(shard_len), new_centers, new_sigmas, log_norm.reshape(1))


def solution(mesh):
    in_specs = (
        P(None, "walk"),
        P(None, "kern"),
        P(None, "kern"),
        P("kern"),
        P("kern"),
        P("walk"),
        P(),
        P(),
    )
    out_specs = (P("walk"), P(None, "walk"), P("kern"), P(None, "kern"), P(None, "kern"), P())
    return jax.shard_map(
        per_device, mesh=mesh, in_specs=in_specs, out_specs=out_specs, check_vma=False
    )
```

```python
import functools
import math

import jax
import jax.numpy as jnp
from jax import lax
from jax.experimental import pallas as pl
from jax.experimental.pallas import tpu as pltpu
from jax.sharding import PartitionSpec as P

PREFACTOR = 0.9
EPSILON = 0.01
RATE = 0.25
LANES = 128
LOG2E = math.log2(math.e)
MESH = pl.DeviceIdType.MESH
F32 = jnp.float32
DIRECT = 2
BF16 = jnp.bfloat16
VMEM = pl.BlockSpec(memory_space=pltpu.VMEM)
HBM = pl.BlockSpec(memory_space=pltpu.HBM)
LIMIT = 24 << 20


def split(x):
    high = x.astype(BF16).astype(F32)
    rest = x - high
    middle = rest.astype(BF16).astype(F32)
    low = (rest - middle).astype(BF16).astype(F32)
    return high, middle, low


def row_of(parts, width):
    row = lax.broadcasted_iota(jnp.int32, (8, width), 0)
    block = jnp.zeros((8, width), F32)
    for index, part in enumerate(parts):
        block = jnp.where(row == index, part, block)
    return block


def sums_kernel(kern_count, walk_count, owners, capacity,
                walkers_hbm, target_hbm, centers_hbm, sigmas_hbm, heights_hbm, live_hbm, norm_hbm, new_sigma_hbm,
                bias_ref, force_ref, new_heights_ref, new_centers_ref, new_sigmas_ref,
                walkers_ref, target_ref, centers_ref, sigmas_ref, heights_ref, live_ref, norm_ref, new_sigma_ref, load_sem,
                walker_feat, kernel_feat, kernel_mom, sums, got, early, early_got, early_far, direct, direct_far,
                mine, shared, far, far_walkers, far_targets, table, placing, spare,
                sent, recv_a, recv_d, recv_e, recv_b, recv_w):
    def load(source, target, index):
        return pltpu.make_async_copy(source, target, load_sem.at[index])

    wide = [
        load(walkers_hbm, walkers_ref, 0),
        load(centers_hbm, centers_ref, 0),
        load(sigmas_hbm, sigmas_ref, 0),
        load(heights_hbm, heights_ref, 0),
        load(target_hbm, target_ref, 0),
    ]
    narrow = [load(live_hbm, live_ref, 1), load(norm_hbm, norm_ref, 2), load(new_sigma_hbm, new_sigma_ref, 3)]
    for copy in wide + narrow:
        copy.start()
    dims, walk_len = walkers_ref.shape
    shard_len = centers_ref.shape[1]
    late = kern_count - owners
    rows = dims + 2
    tail = owners - 2 * DIRECT
    tails = owners - tail
    me = lax.axis_index("kern")
    walk = lax.axis_index("walk")
    flat = me * walk_count + walk
    total_count = kern_count * walk_count

    others = walk_count - 1
    load_rows = (dims * (walk_len + 2 * shard_len) + shard_len + walk_len) // LANES
    walker_rows = others * (dims + 1) * walk_len // LANES

    def other(step):
        return lax.rem(walk + step, walk_count)

    def bulk(count, sem):
        view = spare.at[pl.ds(0, count)]
        return pltpu.make_async_remote_copy(
            src_ref=view, dst_ref=view, send_sem=sent, recv_sem=sem, device_id=(me, walk), device_id_type=MESH
        )

    barrier = pltpu.get_barrier_semaphore()

    def greet(peer):
        pl.semaphore_signal(
            barrier, inc=1, device_id=(peer // walk_count, lax.rem(peer, walk_count)), device_id_type=MESH
        )

    @pl.when(me < owners)
    def _():
        def greet_all(step, carry):
            greet(lax.rem(flat + step, total_count))
            return carry

        lax.fori_loop(1, total_count, greet_all, 0)

    @pl.when(me >= owners)
    def _():
        for step in range(1, walk_count):
            greet(me * walk_count + other(step))

    load(spare.at[pl.ds(0, load_rows)], spare.at[pl.ds(0, load_rows)], 0).wait()
    for copy in narrow:
        copy.wait()
    norm = norm_ref[0]
    walkers = walkers_ref[...]
    sq_h, sq_m, sq_l = split(walkers * walkers)
    wk_h, wk_m, wk_l = split(walkers)
    h, m, l = [sq_h, wk_h], [sq_m, wk_m], [sq_l, wk_l]
    one = jnp.ones((1, walk_len), F32)
    pad = jnp.zeros((LANES - 12 * dims - 8, walk_len), F32)
    stacked = jnp.concatenate(h + m + h + m + l + h + [row_of([one] * 3, walk_len), pad], 0)
    stacked = stacked.astype(BF16)
    width = 2 * LANES
    quarters = walk_len // width
    for quarter in range(quarters):
        walker_feat[quarter] = stacked[:, quarter * width : (quarter + 1) * width]

    centers = centers_ref[...]
    sigmas = sigmas_ref[...]
    inverse_var = 1.0 / (sigmas * sigmas)
    scaled = centers * inverse_var
    constant = jnp.log(heights_ref[...]) - 0.5 * jnp.sum(centers * scaled, 0, keepdims=True)
    k_sq = split((-0.5 * LOG2E) * inverse_var)
    k_lin = split(LOG2E * scaled)
    con = row_of(split(LOG2E * constant), shard_len)
    h, m, l = [[k_sq[i], k_lin[i]] for i in range(3)]
    pad = jnp.zeros((LANES - 12 * dims - 8, shard_len), F32)
    kernel_feat[...] = jnp.concatenate(h + h + m + m + h + l + [con, pad], 0).T.astype(BF16)

    live = live_ref[0]
    alive = (lax.broadcasted_iota(jnp.int32, (8, shard_len), 1) < live).astype(F32)
    mom_a = split(inverse_var * alive)
    mom_c = split(scaled * alive)
    pad = jnp.zeros((8, shard_len), F32)
    mom_rows = [mom_a[0], mom_c[0], mom_a[1], mom_c[1], mom_a[2], mom_c[2], row_of([alive], shard_len), pad]
    kernel_mom[...] = jnp.concatenate(mom_rows, 0).astype(BF16)

    live_row = jnp.full((1, LANES), live, jnp.int32).astype(F32)
    block = min(512, shard_len)

    def copy_a(owner, source):
        return pltpu.make_async_remote_copy(
            src_ref=sums.at[owner], dst_ref=got.at[source],
            send_sem=sent, recv_sem=recv_a.at[0 if owner < tail else jnp.where((me > 0) & (me < owners), 0, 1)],
            device_id=(owner, walk), device_id_type=MESH,
        )

    def copy_d(chunk):
        return pltpu.make_async_remote_copy(
            src_ref=sums.at[pl.ds(chunk, 2)], dst_ref=direct.at[me - owners, pl.ds(chunk - tail, 2)],
            send_sem=sent, recv_sem=recv_d,
            device_id=(0, walk), device_id_type=MESH,
        )

    def copy_g(step, slot, chunk):
        return pltpu.make_async_remote_copy(
            src_ref=sums.at[pl.ds(chunk, 2), pl.ds(dims, 1)], dst_ref=direct_far.at[walk, slot, pl.ds(chunk - tail, 2)],
            send_sem=sent, recv_sem=recv_d,
            device_id=(0, other(step)), device_id_type=MESH,
        )

    def copy_e():
        return pltpu.make_async_remote_copy(
            src_ref=early, dst_ref=early_got.at[me - tail],
            send_sem=sent, recv_sem=recv_e,
            device_id=(0, walk), device_id_type=MESH,
        )

    def copy_h(step):
        return pltpu.make_async_remote_copy(
            src_ref=early.at[pl.ds(dims, 1)], dst_ref=early_far.at[walk, me - tail],
            send_sem=sent, recv_sem=recv_e,
            device_id=(0, other(step)), device_id_type=MESH,
        )

    def copy_b(target, source):
        return pltpu.make_async_remote_copy(
            src_ref=mine, dst_ref=shared.at[source],
            send_sem=sent, recv_sem=recv_b,
            device_id=(target, walk), device_id_type=MESH,
        )

    def copy_c(step, target, source, origin):
        return pltpu.make_async_remote_copy(
            src_ref=mine.at[pl.ds(dims, 1)], dst_ref=far.at[origin, source],
            send_sem=sent, recv_sem=recv_b,
            device_id=(target, other(step)), device_id_type=MESH,
        )

    def copy_w(step, source):
        return (
            pltpu.make_async_remote_copy(
                src_ref=walkers_ref, dst_ref=far_walkers.at[source],
                send_sem=sent, recv_sem=recv_w,
                device_id=(me, other(step)), device_id_type=MESH,
            ),
            pltpu.make_async_remote_copy(
                src_ref=target_ref, dst_ref=far_targets.at[source],
                send_sem=sent, recv_sem=recv_w,
                device_id=(me, other(step)), device_id_type=MESH,
            ),
        )

    def compute(quarter):
        feat = walker_feat[quarter]
        moments = None
        for index in range(shard_len // block):
            part = slice(index * block, (index + 1) * block)
            e = jnp.exp2(jnp.dot(kernel_feat[part, :], feat, preferred_element_type=F32))
            high = e.astype(BF16)
            low = (e - high.astype(F32)).astype(BF16)
            moms = kernel_mom[:, part]
            add = jnp.dot(moms, high, preferred_element_type=F32) + jnp.dot(
                moms, low, preferred_element_type=F32
            )
            moments = add if moments is None else moments + add
        a_sum = moments[0:dims] + moments[2 * dims : 3 * dims] + moments[4 * dims : 5 * dims]
        c_sum = moments[dims : 2 * dims] + moments[3 * dims : 4 * dims] + moments[5 * dims : 6 * dims]
        density = moments[6 * dims : 6 * dims + 1]
        grad = c_sum - walkers_ref[:, quarter * width : (quarter + 1) * width] * a_sum
        for chunk in range(2):
            part = slice(chunk * LANES, (chunk + 1) * LANES)
            sums[quarter * 2 + chunk, 0:dims, :] = grad[:, part]
            sums[quarter * 2 + chunk, dims : dims + 1, :] = density[:, part]
            sums[quarter * 2 + chunk, dims + 1 : dims + 2, :] = live_row

    def sends_a(owner):
        return me != owner

    def send(quarter):
        if 2 * quarter >= tail:
            @pl.when(me >= owners)
            def _():
                copy_d(2 * quarter).start()
                for step in range(1, walk_count):
                    copy_g(step, me - owners, 2 * quarter).start()

            @pl.when(me == 0)
            def _():
                for step in range(1, walk_count):
                    copy_g(step, late, 2 * quarter).start()

        for owner in (2 * quarter, 2 * quarter + 1):
            @pl.when(sends_a(owner))
            def _():
                copy_a(owner, me).start()

    begin = 0
    for end in (quarters // 2, quarters):
        for quarter in range(begin, end):
            compute(quarter)

        @pl.when(me >= owners)
        def _():
            if begin == 0:
                pl.semaphore_wait(barrier, owners * walk_count + others)
            for quarter in range(begin, end):
                send(quarter)

        begin = end

    @pl.when(me < owners)
    def _():
        pl.semaphore_wait(barrier, owners * walk_count - 1)
        for quarter in range(quarters):
            send(quarter)

    for step in range(1, walk_count):
        for copy in copy_w(step, walk):
            copy.start()

    far_walkers[walk] = walkers
    far_targets[walk] = target_ref[...]
    bulk(walker_rows, recv_w).wait_recv()
    targets = [far_targets[index] for index in range(walk_count)]
    if walk_count % 8:
        targets.append(jnp.full((8 - walk_count % 8, walk_len), -1, jnp.int32))
    local = jnp.concatenate(targets, 0) - me * shard_len
    owned = (local >= 0) & (local < shard_len)
    before = lax.broadcasted_iota(jnp.int32, (walk_len, walk_len), 0) < lax.broadcasted_iota(
        jnp.int32, (walk_len, walk_len), 1
    )
    place = jnp.dot(
        jnp.where(owned, 1.0, 0.0).astype(BF16),
        jnp.where(before, 1.0, 0.0).astype(BF16),
        preferred_element_type=F32,
    )
    place = jnp.where(owned, place, -1.0)
    slot = jnp.where(owned, (local + 1).astype(F32), 0.0)
    want = lax.broadcasted_iota(jnp.int32, (capacity, walk_len), 0).astype(F32)

    def pack(feat, index):
        return lax.dot_general(
            feat.astype(BF16), table[index], (((1,), (1,)), ((), ())), preferred_element_type=F32
        )

    slots = lax.broadcasted_iota(jnp.int32, (shard_len, capacity), 0).astype(F32)
    packed_walkers = []
    for index in range(walk_count):
        table[index] = jnp.where(want == place[index : index + 1], 1.0, 0.0).astype(BF16)
        high, middle, low = split(far_walkers[index])
        slot_rows = row_of(split(slot[index : index + 1]), walk_len)
        packed = pack(jnp.concatenate([high, middle, low, slot_rows], 0), index)
        packed_walkers.append(packed[0:dims] + (packed[dims : 2 * dims] + packed[2 * dims : 3 * dims]))
        at = 3 * dims
        packed_slot = packed[at : at + 1] + packed[at + 1 : at + 2] + packed[at + 2 : at + 3] - 1.0
        placing[index] = jnp.where(slots == packed_slot, 1.0, 0.0).astype(BF16)

    def finish(total):
        live_total = total[dims + 1 : dims + 2]
        density = total[dims : dims + 1] / live_total
        ratio = density / norm + EPSILON
        return density, -PREFACTOR * (total[0:dims] / live_total) / (norm * ratio)

    def publish(total, begin):
        density, force = finish(total)
        mine[0:dims, :] = force
        mine[dims : dims + 1, :] = density

        def start_b(target, carry):
            @pl.when(target != me)
            def _():
                copy_b(target, me).start()

            for step in range(1, walk_count):
                copy_c(step, target, me, walk).start()
            return carry

        lax.fori_loop(begin, kern_count, start_b, 0)
        shared[me, 0:dims, :] = force
        shared[me, dims : dims + 1, :] = density

    @pl.when(me < tail)
    def _():
        got[me] = sums[me]
        bulk((kern_count - 1) * rows, recv_a.at[0]).wait_recv()
        total = got[0]
        for source in range(1, kern_count):
            total = total + got[source]
        publish(total, 0)

    @pl.when((me >= tail) & (me < owners))
    def _():
        got[me] = sums[me]
        bulk((owners - 2) * rows, recv_a.at[0]).wait_recv()
        total = got[1]
        for source in range(2, owners):
            total = total + got[source]
        early[...] = total
        copy_e().start()
        for step in range(1, walk_count):
            copy_h(step).start()
        bulk((late + 1) * rows, recv_a.at[1]).wait_recv()
        whole = total + got[0]
        for source in range(owners, kern_count):
            whole = whole + got[source]
        publish(whole, 1)

    @pl.when(me == 0)
    def _():
        bulk((tail - 1) * (dims + 1) + others * tail, recv_b).wait_recv()
        bulk(tails * (rows + others), recv_e).wait_recv()
        bulk(tails * (late * (rows + others) + others), recv_d).wait_recv()
        for index in range(tails):
            whole = early_got[index] + sums[tail + index]
            for source in range(late):
                whole = whole + direct[source, index]
            density, force = finish(whole)
            shared[tail + index, 0:dims, :] = force
            shared[tail + index, dims : dims + 1, :] = density
            for step in range(1, walk_count):
                origin = other(step)
                distant = early_far[origin, index]
                for source in range(late + 1):
                    distant = distant + direct_far[origin, source, index]
                far[origin, tail + index] = distant / whole[dims + 1 : dims + 2]

    @pl.when((me > 0) & (me < owners))
    def _():
        bulk((owners - 1) * (dims + 1) + others * owners, recv_b).wait_recv()

    @pl.when(me >= owners)
    def _():
        bulk(owners * (dims + 1) + others * owners, recv_b).wait_recv()

    def biased(density):
        return PREFACTOR * jnp.log(density / norm + EPSILON)

    for chunk in range(owners):
        part = slice(chunk * LANES, (chunk + 1) * LANES)
        density = shared[chunk, dims : dims + 1, :]
        far[walk, chunk] = density
        bias_ref[:, part] = biased(density)
        force_ref[:, part] = shared[chunk, 0:dims, :]
    density_sum = jnp.zeros((1, 1), F32)
    merged = None
    for index in range(walk_count):
        whole = jnp.concatenate([far[index, chunk] for chunk in range(owners)], 1)
        density_sum = density_sum + jnp.sum(whole, 1, keepdims=True)
        packed = pack(row_of(split(whole), walk_len), index)
        weight = jnp.exp(biased(packed[0:1] + packed[1:2] + packed[2:3]))
        lin = split(weight * packed_walkers[index])
        sq = split(weight * (packed_walkers[index] * packed_walkers[index]))
        last = row_of(split(weight), capacity)
        pad = jnp.zeros((8, capacity), F32)
        feat = jnp.concatenate([lin[0], sq[0], lin[1], sq[1], lin[2], sq[2], last, pad], 0).astype(BF16)
        add = lax.dot_general(feat, placing[index], (((1,), (1,)), ((), ())), preferred_element_type=F32)
        merged = add if merged is None else merged + add
    log_norm = jnp.log((1.0 - RATE) * norm + RATE * density_sum / (walk_len * walk_count))
    bias_ref[:, walk_len : walk_len + LANES] = jnp.broadcast_to(log_norm, (1, LANES))

    first = merged[0:dims] + (merged[2 * dims : 3 * dims] + merged[4 * dims : 5 * dims])
    second = merged[dims : 2 * dims] + (merged[3 * dims : 4 * dims] + merged[5 * dims : 6 * dims])
    at = 6 * dims
    gain = merged[at : at + 1] + (merged[at + 1 : at + 2] + merged[at + 2 : at + 3])
    row = lax.broadcasted_iota(jnp.int32, (dims, dims), 0)
    column = lax.broadcasted_iota(jnp.int32, (dims, dims), 1)
    new_sigma = jnp.sum(jnp.where(row == column, new_sigma_ref[...], 0.0), 1, keepdims=True)
    centers = centers_ref[...]
    sigmas = sigmas_ref[...]
    heights = heights_ref[...]
    shift = first - centers * gain
    spread = second - 2.0 * centers * first + centers * centers * gain + new_sigma * new_sigma * gain
    new_heights = heights + gain
    delta = shift / new_heights
    new_heights_ref[...] = new_heights
    new_centers_ref[...] = centers + delta
    new_sigmas_ref[...] = jnp.sqrt((heights * sigmas * sigmas + spread) / new_heights - delta * delta)

    always = walker_rows + (owners - 1) * rows

    @pl.when(me >= owners)
    def _():
        bulk(always + rows + tails * (rows + others), sent).wait_send()

    @pl.when((me > 0) & (me < tail))
    def _():
        bulk(always + (kern_count - 1) * (dims + 1) + others * kern_count, sent).wait_send()

    @pl.when(me == 0)
    def _():
        bulk(always + (kern_count - 1) * (dims + 1) + others * (kern_count + tails), sent).wait_send()

    @pl.when((me >= tail) & (me < owners))
    def _():
        bulk(always + rows + (kern_count - 2) * (dims + 1) + others * kern_count, sent).wait_send()


def write_kernel(bias_ref, force_ref, new_heights_ref, new_centers_ref, new_sigmas_ref,
                 bias_hbm, force_hbm, new_heights_hbm, new_centers_hbm, new_sigmas_hbm, log_norm_hbm, log_norm_ref, sem):
    walk_len = bias_hbm.shape[1]
    log_norm_ref[...] = bias_ref[:, walk_len : walk_len + 1]
    pairs = [
        (new_centers_ref, new_centers_hbm),
        (new_sigmas_ref, new_sigmas_hbm),
        (force_ref, force_hbm),
        (new_heights_ref, new_heights_hbm),
        (bias_ref.at[:, pl.ds(0, walk_len)], bias_hbm),
        (log_norm_ref, log_norm_hbm),
    ]
    copies = [pltpu.make_async_copy(source, target, sem.at[index]) for index, (source, target) in enumerate(pairs)]
    for copy in copies:
        copy.start()
    for copy in copies:
        copy.wait()


def per_device(walkers, centers, sigmas, heights, kernel_live, merge_target, new_sigma, norm_old):
    dims, walk_len = walkers.shape
    shard_len = centers.shape[1]
    kern_count = lax.axis_size("kern")
    walk_count = lax.axis_size("walk")
    owners = walk_len // LANES
    late = kern_count - owners
    quarters = owners // 2
    rows = dims + 2
    capacity = 2 * walk_len // kern_count
    height_row = heights.reshape(1, shard_len)
    load_rows = (dims * (walk_len + 2 * shard_len) + shard_len + walk_len) // LANES
    walker_rows = walk_count * (dims + 1) * walk_len // LANES
    answer_rows = walk_count * kern_count + kern_count * rows
    spare_rows = load_rows + walker_rows + answer_rows + kern_count * owners * (rows + walk_count)

    dma = pltpu.SemaphoreType.DMA
    shapes = [(1, walk_len), (dims, walk_len), (1, shard_len), (dims, shard_len), (dims, shard_len), (1, 1)]
    results = pl.pallas_call(
        functools.partial(sums_kernel, kern_count, walk_count, owners, capacity),
        out_shape=[pltpu.VMEM(shape, F32) for shape in [(1, walk_len + LANES)] + shapes[1:5]],
        in_specs=[HBM] * 8,
        scratch_shapes=[
            pltpu.VMEM((dims, walk_len), F32),
            pltpu.VMEM((1, walk_len), jnp.int32),
            pltpu.VMEM((dims, shard_len), F32),
            pltpu.VMEM((dims, shard_len), F32),
            pltpu.VMEM((1, shard_len), F32),
            pltpu.SMEM((1,), jnp.int32),
            pltpu.SMEM((1,), F32),
            pltpu.VMEM((1, dims), F32),
            dma((4,)),
            pltpu.VMEM((walk_len // (2 * LANES), LANES, 2 * LANES), BF16),
            pltpu.VMEM((shard_len, LANES), BF16),
            pltpu.VMEM((6 * dims + 16, shard_len), BF16),
            pltpu.VMEM((owners, rows, LANES), F32),
            pltpu.VMEM((kern_count, rows, LANES), F32),
            pltpu.VMEM((rows, LANES), F32),
            pltpu.VMEM((2 * DIRECT, rows, LANES), F32),
            pltpu.VMEM((walk_count, 2 * DIRECT, 1, LANES), F32),
            pltpu.VMEM((late, 2 * DIRECT, rows, LANES), F32),
            pltpu.VMEM((walk_count, late + 1, 2 * DIRECT, 1, LANES), F32),
            pltpu.VMEM((dims + 1, LANES), F32),
            pltpu.VMEM((owners, dims + 1, LANES), F32),
            pltpu.VMEM((walk_count, owners, 1, LANES), F32),
            pltpu.VMEM((walk_count, dims, walk_len), F32),
            pltpu.VMEM((walk_count, 1, walk_len), jnp.int32),
            pltpu.VMEM((walk_count, capacity, walk_len), BF16),
            pltpu.VMEM((walk_count, shard_len, capacity), BF16),
            pltpu.VMEM((spare_rows, LANES), F32),
            dma, dma((2,)), dma, dma, dma, dma,
        ],
        compiler_params=pltpu.CompilerParams(collective_id=0, has_side_effects=True, vmem_limit_bytes=LIMIT),
        name="sums",
    )(*[
        pltpu.with_memory_space_constraint(x, pltpu.HBM)
        for x in (walkers, merge_target.reshape(1, walk_len), centers, sigmas, height_row)
    ], kernel_live, norm_old, pltpu.with_memory_space_constraint(new_sigma.reshape(1, dims), pltpu.HBM))

    bias, force, new_heights, new_centers, new_sigmas, log_norm = pl.pallas_call(
        write_kernel,
        out_shape=[jax.ShapeDtypeStruct(shape, F32) for shape in shapes],
        in_specs=[VMEM] * 5,
        out_specs=[HBM] * 6,
        scratch_shapes=[pltpu.VMEM((1, 1), F32), dma((6,))],
        compiler_params=pltpu.CompilerParams(vmem_limit_bytes=LIMIT),
        name="write",
    )(*results)
    return (bias.reshape(walk_len), force, new_heights.reshape(shard_len), new_centers, new_sigmas, log_norm.reshape(1))


def solution(mesh):
    in_specs = (
        P(None, "walk"),
        P(None, "kern"),
        P(None, "kern"),
        P("kern"),
        P("kern"),
        P("walk"),
        P(),
        P(),
    )
    out_specs = (P("walk"), P(None, "walk"), P("kern"), P(None, "kern"), P(None, "kern"), P())
    return jax.shard_map(
        per_device, mesh=mesh, in_specs=in_specs, out_specs=out_specs, check_vma=False
    )
```

```python
import functools
import math

import jax
import jax.numpy as jnp
from jax import lax
from jax.experimental import pallas as pl
from jax.experimental.pallas import tpu as pltpu
from jax.sharding import PartitionSpec as P

PREFACTOR = 0.9
EPSILON = 0.01
RATE = 0.25
LANES = 128
LOG2E = math.log2(math.e)
MESH = pl.DeviceIdType.MESH
F32 = jnp.float32
DIRECT = 2
BF16 = jnp.bfloat16
VMEM = pl.BlockSpec(memory_space=pltpu.VMEM)
HBM = pl.BlockSpec(memory_space=pltpu.HBM)
LIMIT = 24 << 20


def split(x):
    high = x.astype(BF16).astype(F32)
    rest = x - high
    middle = rest.astype(BF16).astype(F32)
    low = (rest - middle).astype(BF16).astype(F32)
    return high, middle, low


def row_of(parts, width):
    row = lax.broadcasted_iota(jnp.int32, (8, width), 0)
    block = jnp.zeros((8, width), F32)
    for index, part in enumerate(parts):
        block = jnp.where(row == index, part, block)
    return block


def sums_kernel(kern_count, walk_count, owners, capacity,
                walkers_hbm, target_hbm, centers_hbm, sigmas_hbm, heights_hbm, live_hbm, norm_hbm, new_sigma_hbm,
                bias_ref, force_ref, new_heights_ref, new_centers_ref, new_sigmas_ref,
                walkers_ref, target_ref, centers_ref, sigmas_ref, heights_ref, live_ref, norm_ref, new_sigma_ref, load_sem,
                walker_feat, kernel_feat, kernel_mom, sums, got, early, early_got, early_far, direct, direct_far,
                mine, shared, far, far_walkers, far_targets, table, placing, spare,
                sent, recv_a, recv_d, recv_e, recv_b, recv_w):
    def load(source, target, index):
        return pltpu.make_async_copy(source, target, load_sem.at[index])

    wide = [
        load(walkers_hbm, walkers_ref, 0),
        load(centers_hbm, centers_ref, 0),
        load(sigmas_hbm, sigmas_ref, 0),
        load(heights_hbm, heights_ref, 0),
        load(target_hbm, target_ref, 0),
    ]
    narrow = [load(live_hbm, live_ref, 1), load(norm_hbm, norm_ref, 2), load(new_sigma_hbm, new_sigma_ref, 3)]
    for copy in wide + narrow:
        copy.start()
    dims, walk_len = walkers_ref.shape
    shard_len = centers_ref.shape[1]
    late = kern_count - owners
    rows = dims + 2
    tail = owners - 2 * DIRECT
    tails = owners - tail
    me = lax.axis_index("kern")
    walk = lax.axis_index("walk")
    flat = me * walk_count + walk
    total_count = kern_count * walk_count

    others = walk_count - 1
    load_rows = (dims * (walk_len + 2 * shard_len) + shard_len + walk_len) // LANES
    walker_rows = others * (dims + 1) * walk_len // LANES

    def other(step):
        return lax.rem(walk + step, walk_count)

    def bulk(count, sem):
        view = spare.at[pl.ds(0, count)]
        return pltpu.make_async_remote_copy(
            src_ref=view, dst_ref=view, send_sem=sent, recv_sem=sem, device_id=(me, walk), device_id_type=MESH
        )

    barrier = pltpu.get_barrier_semaphore()

    def greet(peer):
        pl.semaphore_signal(
            barrier, inc=1, device_id=(peer // walk_count, lax.rem(peer, walk_count)), device_id_type=MESH
        )

    @pl.when(me < owners)
    def _():
        def greet_all(step, carry):
            greet(lax.rem(flat + step, total_count))
            return carry

        lax.fori_loop(1, total_count, greet_all, 0)

    @pl.when(me >= owners)
    def _():
        for step in range(1, walk_count):
            greet(me * walk_count + other(step))

    load(spare.at[pl.ds(0, load_rows)], spare.at[pl.ds(0, load_rows)], 0).wait()
    for copy in narrow:
        copy.wait()
    norm = norm_ref[0]
    walkers = walkers_ref[...]
    sq_h, sq_m, sq_l = split(walkers * walkers)
    wk_h, wk_m, wk_l = split(walkers)
    h, m, l = [sq_h, wk_h], [sq_m, wk_m], [sq_l, wk_l]
    one = jnp.ones((1, walk_len), F32)
    pad = jnp.zeros((LANES - 12 * dims - 8, walk_len), F32)
    stacked = jnp.concatenate(h + m + h + m + l + h + [row_of([one] * 3, walk_len), pad], 0)
    stacked = stacked.astype(BF16)
    width = 2 * LANES
    quarters = walk_len // width
    for quarter in range(quarters):
        walker_feat[quarter] = stacked[:, quarter * width : (quarter + 1) * width]

    centers = centers_ref[...]
    sigmas = sigmas_ref[...]
    inverse_var = 1.0 / (sigmas * sigmas)
    scaled = centers * inverse_var
    constant = jnp.log(heights_ref[...]) - 0.5 * jnp.sum(centers * scaled, 0, keepdims=True)
    k_sq = split((-0.5 * LOG2E) * inverse_var)
    k_lin = split(LOG2E * scaled)
    con = row_of(split(LOG2E * constant), shard_len)
    h, m, l = [[k_sq[i], k_lin[i]] for i in range(3)]
    pad = jnp.zeros((LANES - 12 * dims - 8, shard_len), F32)
    kernel_feat[...] = jnp.concatenate(h + h + m + m + h + l + [con, pad], 0).T.astype(BF16)

    live = live_ref[0]
    alive = (lax.broadcasted_iota(jnp.int32, (8, shard_len), 1) < live).astype(F32)
    mom_a = split(inverse_var * alive)
    mom_c = split(scaled * alive)
    pad = jnp.zeros((8, shard_len), F32)
    mom_rows = [mom_a[0], mom_c[0], mom_a[1], mom_c[1], mom_a[2], mom_c[2], row_of([alive], shard_len), pad]
    kernel_mom[...] = jnp.concatenate(mom_rows, 0).astype(BF16)

    live_row = jnp.full((1, LANES), live, jnp.int32).astype(F32)
    block = min(512, shard_len)

    def copy_a(owner, source):
        return pltpu.make_async_remote_copy(
            src_ref=sums.at[owner], dst_ref=got.at[source],
            send_sem=sent, recv_sem=recv_a.at[0 if owner < tail else jnp.where((me > 0) & (me < owners), 0, 1)],
            device_id=(owner, walk), device_id_type=MESH,
        )

    def copy_d(chunk):
        return pltpu.make_async_remote_copy(
            src_ref=sums.at[pl.ds(chunk, 2)], dst_ref=direct.at[me - owners, pl.ds(chunk - tail, 2)],
            send_sem=sent, recv_sem=recv_d,
            device_id=(0, walk), device_id_type=MESH,
        )

    def copy_g(step, slot, chunk):
        return pltpu.make_async_remote_copy(
            src_ref=sums.at[pl.ds(chunk, 2), pl.ds(dims, 1)], dst_ref=direct_far.at[walk, slot, pl.ds(chunk - tail, 2)],
            send_sem=sent, recv_sem=recv_d,
            device_id=(0, other(step)), device_id_type=MESH,
        )

    def copy_e():
        return pltpu.make_async_remote_copy(
            src_ref=early, dst_ref=early_got.at[me - tail],
            send_sem=sent, recv_sem=recv_e,
            device_id=(0, walk), device_id_type=MESH,
        )

    def copy_h(step):
        return pltpu.make_async_remote_copy(
            src_ref=early.at[pl.ds(dims, 1)], dst_ref=early_far.at[walk, me - tail],
            send_sem=sent, recv_sem=recv_e,
            device_id=(0, other(step)), device_id_type=MESH,
        )

    def copy_b(target, source):
        return pltpu.make_async_remote_copy(
            src_ref=mine, dst_ref=shared.at[source],
            send_sem=sent, recv_sem=recv_b,
            device_id=(target, walk), device_id_type=MESH,
        )

    def copy_c(step, target, source, origin):
        return pltpu.make_async_remote_copy(
            src_ref=mine.at[pl.ds(dims, 1)], dst_ref=far.at[origin, source],
            send_sem=sent, recv_sem=recv_b,
            device_id=(target, other(step)), device_id_type=MESH,
        )

    def copy_w(step, source):
        return (
            pltpu.make_async_remote_copy(
                src_ref=walkers_ref, dst_ref=far_walkers.at[source],
                send_sem=sent, recv_sem=recv_w,
                device_id=(me, other(step)), device_id_type=MESH,
            ),
            pltpu.make_async_remote_copy(
                src_ref=target_ref, dst_ref=far_targets.at[source],
                send_sem=sent, recv_sem=recv_w,
                device_id=(me, other(step)), device_id_type=MESH,
            ),
        )

    def compute(quarter):
        feat = walker_feat[quarter]
        moments = None
        for index in range(shard_len // block):
            part = slice(index * block, (index + 1) * block)
            e = jnp.exp2(jnp.dot(kernel_feat[part, :], feat, preferred_element_type=F32))
            high = e.astype(BF16)
            low = (e - high.astype(F32)).astype(BF16)
            moms = kernel_mom[:, part]
            add = jnp.dot(moms, high, preferred_element_type=F32) + jnp.dot(
                moms, low, preferred_element_type=F32
            )
            moments = add if moments is None else moments + add
        a_sum = moments[0:dims] + moments[2 * dims : 3 * dims] + moments[4 * dims : 5 * dims]
        c_sum = moments[dims : 2 * dims] + moments[3 * dims : 4 * dims] + moments[5 * dims : 6 * dims]
        density = moments[6 * dims : 6 * dims + 1]
        grad = c_sum - walkers_ref[:, quarter * width : (quarter + 1) * width] * a_sum
        for chunk in range(2):
            part = slice(chunk * LANES, (chunk + 1) * LANES)
            sums[quarter * 2 + chunk, 0:dims, :] = grad[:, part]
            sums[quarter * 2 + chunk, dims : dims + 1, :] = density[:, part]
            sums[quarter * 2 + chunk, dims + 1 : dims + 2, :] = live_row

    def sends_a(owner):
        return me != owner

    def send(quarter):
        if 2 * quarter >= tail:
            @pl.when(me >= owners)
            def _():
                copy_d(2 * quarter).start()
                for step in range(1, walk_count):
                    copy_g(step, me - owners, 2 * quarter).start()

            @pl.when(me == 0)
            def _():
                for step in range(1, walk_count):
                    copy_g(step, late, 2 * quarter).start()

        for owner in (2 * quarter, 2 * quarter + 1):
            @pl.when(sends_a(owner))
            def _():
                copy_a(owner, me).start()

    begin = 0
    for end in (quarters // 2, quarters):
        for quarter in range(begin, end):
            compute(quarter)

        @pl.when(me >= owners)
        def _():
            if begin == 0:
                pl.semaphore_wait(barrier, owners * walk_count + others)
            for quarter in range(begin, end):
                send(quarter)

        begin = end

    @pl.when(me < owners)
    def _():
        pl.semaphore_wait(barrier, owners * walk_count - 1)
        for quarter in range(quarters):
            send(quarter)

    for step in range(1, walk_count):
        for copy in copy_w(step, walk):
            copy.start()

    far_walkers[walk] = walkers
    far_targets[walk] = target_ref[...]
    bulk(walker_rows, recv_w).wait_recv()
    targets = [far_targets[index] for index in range(walk_count)]
    if walk_count % 8:
        targets.append(jnp.full((8 - walk_count % 8, walk_len), -1, jnp.int32))
    local = jnp.concatenate(targets, 0) - me * shard_len
    owned = (local >= 0) & (local < shard_len)
    before = lax.broadcasted_iota(jnp.int32, (walk_len, walk_len), 0) < lax.broadcasted_iota(
        jnp.int32, (walk_len, walk_len), 1
    )
    place = jnp.dot(
        jnp.where(owned, 1.0, 0.0).astype(BF16),
        jnp.where(before, 1.0, 0.0).astype(BF16),
        preferred_element_type=F32,
    )
    slot = jnp.where(owned, (local + 1).astype(F32), 0.0)

    def pack(feat):
        return jnp.dot(feat.astype(BF16), table[...], preferred_element_type=F32)

    def of_walk(index, height):
        column = lax.broadcasted_iota(jnp.int32, (height, span), 1)
        return (column >= index * capacity) & (column < (index + 1) * capacity)

    span = walk_count * capacity
    lane = lax.broadcasted_iota(jnp.int32, (walk_len, LANES), 1).astype(F32)
    spots = [
        jnp.broadcast_to(jnp.where(owned[index : index + 1], place[index : index + 1] + index * capacity, -1.0), (LANES, walk_len)).T
        for index in range(walk_count)
    ]
    for at in range(0, span, LANES):
        hit = lane + at == spots[0]
        for spot in spots[1:]:
            hit = hit | (lane + at == spot)
        table[:, at : at + LANES] = jnp.where(hit, 1.0, 0.0).astype(BF16)
    packed = jnp.zeros((3 * dims + 8, span), F32)
    for index in range(walk_count):
        high, middle, low = split(far_walkers[index])
        slot_rows = row_of(split(slot[index : index + 1]), walk_len)
        found = pack(jnp.concatenate([high, middle, low, slot_rows], 0))
        packed = jnp.where(of_walk(index, 3 * dims + 8), found, packed)
    packed_walkers = packed[0:dims] + (packed[dims : 2 * dims] + packed[2 * dims : 3 * dims])
    at = 3 * dims
    packed_slot = packed[at : at + 1] + packed[at + 1 : at + 2] + packed[at + 2 : at + 3] - 1.0
    target_slot = jnp.broadcast_to(packed_slot, (LANES, span)).T
    lane = lax.broadcasted_iota(jnp.int32, (span, LANES), 1).astype(F32)
    for at in range(0, shard_len, LANES):
        placing[:, at : at + LANES] = jnp.where(lane + at == target_slot, 1.0, 0.0).astype(BF16)
    height = (3 * walk_count + 7) // 8 * 8
    row = lax.broadcasted_iota(jnp.int32, (height, span), 0)
    own = jnp.zeros((height, span), jnp.bool_)
    for index in range(walk_count):
        own = own | (of_walk(index, height) & (row >= 3 * index) & (row < 3 * index + 3))
    packed_squares = packed_walkers * packed_walkers

    def finish(total):
        live_total = total[dims + 1 : dims + 2]
        density = total[dims : dims + 1] / live_total
        ratio = density / norm + EPSILON
        return density, -PREFACTOR * (total[0:dims] / live_total) / (norm * ratio)

    def publish(total, begin):
        density, force = finish(total)
        mine[0:dims, :] = force
        mine[dims : dims + 1, :] = density

        def start_b(target, carry):
            @pl.when(target != me)
            def _():
                copy_b(target, me).start()

            for step in range(1, walk_count):
                copy_c(step, target, me, walk).start()
            return carry

        lax.fori_loop(begin, kern_count, start_b, 0)
        shared[me, 0:dims, :] = force
        shared[me, dims : dims + 1, :] = density

    @pl.when(me < tail)
    def _():
        got[me] = sums[me]
        bulk((kern_count - 1) * rows, recv_a.at[0]).wait_recv()
        total = got[0]
        for source in range(1, kern_count):
            total = total + got[source]
        publish(total, 0)

    @pl.when((me >= tail) & (me < owners))
    def _():
        got[me] = sums[me]
        bulk((owners - 2) * rows, recv_a.at[0]).wait_recv()
        total = got[1]
        for source in range(2, owners):
            total = total + got[source]
        early[...] = total
        copy_e().start()
        for step in range(1, walk_count):
            copy_h(step).start()
        bulk((late + 1) * rows, recv_a.at[1]).wait_recv()
        whole = total + got[0]
        for source in range(owners, kern_count):
            whole = whole + got[source]
        publish(whole, 1)

    @pl.when(me == 0)
    def _():
        bulk((tail - 1) * (dims + 1) + others * tail, recv_b).wait_recv()
        bulk(tails * (rows + others), recv_e).wait_recv()
        bulk(tails * (late * (rows + others) + others), recv_d).wait_recv()
        for index in range(tails):
            whole = early_got[index] + sums[tail + index]
            for source in range(late):
                whole = whole + direct[source, index]
            density, force = finish(whole)
            shared[tail + index, 0:dims, :] = force
            shared[tail + index, dims : dims + 1, :] = density
            for step in range(1, walk_count):
                origin = other(step)
                distant = early_far[origin, index]
                for source in range(late + 1):
                    distant = distant + direct_far[origin, source, index]
                far[origin, tail + index] = distant / whole[dims + 1 : dims + 2]

    @pl.when((me > 0) & (me < owners))
    def _():
        bulk((owners - 1) * (dims + 1) + others * owners, recv_b).wait_recv()

    @pl.when(me >= owners)
    def _():
        bulk(owners * (dims + 1) + others * owners, recv_b).wait_recv()

    def biased(density):
        return PREFACTOR * jnp.log(density / norm + EPSILON)

    for chunk in range(owners):
        part = slice(chunk * LANES, (chunk + 1) * LANES)
        density = shared[chunk, dims : dims + 1, :]
        far[walk, chunk] = density
        bias_ref[:, part] = biased(density)
        force_ref[:, part] = shared[chunk, 0:dims, :]
    density_sum = jnp.zeros((1, 1), F32)
    line = lax.broadcasted_iota(jnp.int32, (height, walk_len), 0)
    lines = jnp.zeros((height, walk_len), F32)
    for index in range(walk_count):
        whole = jnp.concatenate([far[index, chunk] for chunk in range(owners)], 1)
        density_sum = density_sum + jnp.sum(whole, 1, keepdims=True)
        for part, value in enumerate(split(whole)):
            lines = jnp.where(line == 3 * index + part, value, lines)
    weight = jnp.exp(biased(jnp.sum(jnp.where(own, pack(lines), 0.0), 0, keepdims=True)))
    lin = split(weight * packed_walkers)
    sq = split(weight * packed_squares)
    last = row_of(split(weight), span)
    pad = jnp.zeros((8, span), F32)
    feat = jnp.concatenate([lin[0], sq[0], lin[1], sq[1], lin[2], sq[2], last, pad], 0).astype(BF16)
    merged = jnp.dot(feat, placing[...], preferred_element_type=F32)
    log_norm = jnp.log((1.0 - RATE) * norm + RATE * density_sum / (walk_len * walk_count))
    bias_ref[:, walk_len : walk_len + LANES] = jnp.broadcast_to(log_norm, (1, LANES))

    first = merged[0:dims] + (merged[2 * dims : 3 * dims] + merged[4 * dims : 5 * dims])
    second = merged[dims : 2 * dims] + (merged[3 * dims : 4 * dims] + merged[5 * dims : 6 * dims])
    at = 6 * dims
    gain = merged[at : at + 1] + (merged[at + 1 : at + 2] + merged[at + 2 : at + 3])
    row = lax.broadcasted_iota(jnp.int32, (dims, dims), 0)
    column = lax.broadcasted_iota(jnp.int32, (dims, dims), 1)
    new_sigma = jnp.sum(jnp.where(row == column, new_sigma_ref[...], 0.0), 1, keepdims=True)
    centers = centers_ref[...]
    sigmas = sigmas_ref[...]
    heights = heights_ref[...]
    shift = first - centers * gain
    spread = second - 2.0 * centers * first + centers * centers * gain + new_sigma * new_sigma * gain
    new_heights = heights + gain
    inverse = 1.0 / new_heights
    delta = shift * inverse
    new_heights_ref[...] = new_heights
    new_centers_ref[...] = centers + delta
    new_sigmas_ref[...] = jnp.sqrt((heights * sigmas * sigmas + spread) * inverse - delta * delta)

    always = walker_rows + (owners - 1) * rows

    @pl.when(me >= owners)
    def _():
        bulk(always + rows + tails * (rows + others), sent).wait_send()

    @pl.when((me > 0) & (me < tail))
    def _():
        bulk(always + (kern_count - 1) * (dims + 1) + others * kern_count, sent).wait_send()

    @pl.when(me == 0)
    def _():
        bulk(always + (kern_count - 1) * (dims + 1) + others * (kern_count + tails), sent).wait_send()

    @pl.when((me >= tail) & (me < owners))
    def _():
        bulk(always + rows + (kern_count - 2) * (dims + 1) + others * kern_count, sent).wait_send()


def write_kernel(bias_ref, force_ref, new_heights_ref, new_centers_ref, new_sigmas_ref,
                 bias_hbm, force_hbm, new_heights_hbm, new_centers_hbm, new_sigmas_hbm, log_norm_hbm, log_norm_ref, sem):
    walk_len = bias_hbm.shape[1]
    log_norm_ref[...] = bias_ref[:, walk_len : walk_len + 1]
    pairs = [
        (new_centers_ref, new_centers_hbm),
        (new_sigmas_ref, new_sigmas_hbm),
        (force_ref, force_hbm),
        (new_heights_ref, new_heights_hbm),
        (bias_ref.at[:, pl.ds(0, walk_len)], bias_hbm),
        (log_norm_ref, log_norm_hbm),
    ]
    copies = [pltpu.make_async_copy(source, target, sem.at[index]) for index, (source, target) in enumerate(pairs)]
    for copy in copies:
        copy.start()
    for copy in copies:
        copy.wait()


def per_device(walkers, centers, sigmas, heights, kernel_live, merge_target, new_sigma, norm_old):
    dims, walk_len = walkers.shape
    shard_len = centers.shape[1]
    kern_count = lax.axis_size("kern")
    walk_count = lax.axis_size("walk")
    owners = walk_len // LANES
    late = kern_count - owners
    quarters = owners // 2
    rows = dims + 2
    capacity = 2 * walk_len // kern_count
    height_row = heights.reshape(1, shard_len)
    load_rows = (dims * (walk_len + 2 * shard_len) + shard_len + walk_len) // LANES
    walker_rows = walk_count * (dims + 1) * walk_len // LANES
    answer_rows = walk_count * kern_count + kern_count * rows
    spare_rows = load_rows + walker_rows + answer_rows + kern_count * owners * (rows + walk_count)

    dma = pltpu.SemaphoreType.DMA
    shapes = [(1, walk_len), (dims, walk_len), (1, shard_len), (dims, shard_len), (dims, shard_len), (1, 1)]
    results = pl.pallas_call(
        functools.partial(sums_kernel, kern_count, walk_count, owners, capacity),
        out_shape=[pltpu.VMEM(shape, F32) for shape in [(1, walk_len + LANES)] + shapes[1:5]],
        in_specs=[HBM] * 8,
        scratch_shapes=[
            pltpu.VMEM((dims, walk_len), F32),
            pltpu.VMEM((1, walk_len), jnp.int32),
            pltpu.VMEM((dims, shard_len), F32),
            pltpu.VMEM((dims, shard_len), F32),
            pltpu.VMEM((1, shard_len), F32),
            pltpu.SMEM((1,), jnp.int32),
            pltpu.SMEM((1,), F32),
            pltpu.VMEM((1, dims), F32),
            dma((4,)),
            pltpu.VMEM((walk_len // (2 * LANES), LANES, 2 * LANES), BF16),
            pltpu.VMEM((shard_len, LANES), BF16),
            pltpu.VMEM((6 * dims + 16, shard_len), BF16),
            pltpu.VMEM((owners, rows, LANES), F32),
            pltpu.VMEM((kern_count, rows, LANES), F32),
            pltpu.VMEM((rows, LANES), F32),
            pltpu.VMEM((2 * DIRECT, rows, LANES), F32),
            pltpu.VMEM((walk_count, 2 * DIRECT, 1, LANES), F32),
            pltpu.VMEM((late, 2 * DIRECT, rows, LANES), F32),
            pltpu.VMEM((walk_count, late + 1, 2 * DIRECT, 1, LANES), F32),
            pltpu.VMEM((dims + 1, LANES), F32),
            pltpu.VMEM((owners, dims + 1, LANES), F32),
            pltpu.VMEM((walk_count, owners, 1, LANES), F32),
            pltpu.VMEM((walk_count, dims, walk_len), F32),
            pltpu.VMEM((walk_count, 1, walk_len), jnp.int32),
            pltpu.VMEM((walk_len, walk_count * capacity), BF16),
            pltpu.VMEM((walk_count * capacity, shard_len), BF16),
            pltpu.VMEM((spare_rows, LANES), F32),
            dma, dma((2,)), dma, dma, dma, dma,
        ],
        compiler_params=pltpu.CompilerParams(collective_id=0, has_side_effects=True, vmem_limit_bytes=LIMIT),
        name="sums",
    )(*[
        pltpu.with_memory_space_constraint(x, pltpu.HBM)
        for x in (walkers, merge_target.reshape(1, walk_len), centers, sigmas, height_row)
    ], kernel_live, norm_old, pltpu.with_memory_space_constraint(new_sigma.reshape(1, dims), pltpu.HBM))

    bias, force, new_heights, new_centers, new_sigmas, log_norm = pl.pallas_call(
        write_kernel,
        out_shape=[jax.ShapeDtypeStruct(shape, F32) for shape in shapes],
        in_specs=[VMEM] * 5,
        out_specs=[HBM] * 6,
        scratch_shapes=[pltpu.VMEM((1, 1), F32), dma((6,))],
        compiler_params=pltpu.CompilerParams(vmem_limit_bytes=LIMIT),
        name="write",
    )(*results)
    return (bias.reshape(walk_len), force, new_heights.reshape(shard_len), new_centers, new_sigmas, log_norm.reshape(1))


def solution(mesh):
    in_specs = (
        P(None, "walk"),
        P(None, "kern"),
        P(None, "kern"),
        P("kern"),
        P("kern"),
        P("walk"),
        P(),
        P(),
    )
    out_specs = (P("walk"), P(None, "walk"), P("kern"), P(None, "kern"), P(None, "kern"), P())
    return jax.shard_map(
        per_device, mesh=mesh, in_specs=in_specs, out_specs=out_specs, check_vma=False
    )
```

```python
import functools
import math

import jax
import jax.numpy as jnp
from jax import lax
from jax.experimental import pallas as pl
from jax.experimental.pallas import tpu as pltpu
from jax.sharding import PartitionSpec as P

PREFACTOR = 0.9
EPSILON = 0.01
RATE = 0.25
LANES = 128
LOG2E = math.log2(math.e)
MESH = pl.DeviceIdType.MESH
F32 = jnp.float32
DIRECT = 2
BF16 = jnp.bfloat16
VMEM = pl.BlockSpec(memory_space=pltpu.VMEM)
HBM = pl.BlockSpec(memory_space=pltpu.HBM)
LIMIT = 24 << 20


def split(x):
    high = x.astype(BF16).astype(F32)
    rest = x - high
    middle = rest.astype(BF16).astype(F32)
    low = (rest - middle).astype(BF16).astype(F32)
    return high, middle, low


def row_of(parts, width):
    row = lax.broadcasted_iota(jnp.int32, (8, width), 0)
    block = jnp.zeros((8, width), F32)
    for index, part in enumerate(parts):
        block = jnp.where(row == index, part, block)
    return block


def sums_kernel(kern_count, walk_count, owners, capacity,
                walkers_hbm, target_hbm, centers_hbm, sigmas_hbm, heights_hbm, live_hbm, norm_hbm, new_sigma_hbm,
                bias_ref, force_ref, new_heights_ref, new_centers_ref, new_sigmas_ref,
                walkers_ref, target_ref, centers_ref, sigmas_ref, heights_ref, live_ref, norm_ref, new_sigma_ref, load_sem,
                walker_feat, kernel_feat, kernel_mom, sums, got, direct, direct_far,
                mine, shared, far, far_walkers, far_targets, table, placing, spare,
                sent, recv_a, recv_d, recv_b, recv_w):
    def load(source, target, index):
        return pltpu.make_async_copy(source, target, load_sem.at[index])

    wide = [
        load(walkers_hbm, walkers_ref, 0),
        load(centers_hbm, centers_ref, 0),
        load(sigmas_hbm, sigmas_ref, 0),
        load(heights_hbm, heights_ref, 0),
        load(target_hbm, target_ref, 0),
    ]
    narrow = [load(live_hbm, live_ref, 1), load(norm_hbm, norm_ref, 2), load(new_sigma_hbm, new_sigma_ref, 3)]
    for copy in wide + narrow:
        copy.start()
    dims, walk_len = walkers_ref.shape
    shard_len = centers_ref.shape[1]
    rows = dims + 2
    me = lax.axis_index("kern")
    walk = lax.axis_index("walk")
    flat = me * walk_count + walk
    total_count = kern_count * walk_count
    quarters = owners // 2
    head = quarters - DIRECT
    half = quarters // 2
    holders = [quarter + 1 for quarter in range(half)] + [
        kern_count - 1 - (quarter + 1 - half) * (kern_count // quarters) for quarter in range(half, quarters)
    ]
    mine_quarter = 0
    for quarter in range(1, quarters):
        mine_quarter = jnp.where(me == holders[quarter], quarter, mine_quarter)
    owns = me == holders[0]
    for holder in holders[1:]:
        owns = owns | (me == holder)
    owns_head = owns & (mine_quarter < head)
    owns_tail = owns & (mine_quarter >= head)
    greets = owns | (me == 0)
    greeted = (quarters + 1) * walk_count

    others = walk_count - 1
    load_rows = (dims * (walk_len + 2 * shard_len) + shard_len + walk_len) // LANES
    walker_rows = others * (dims + 1) * walk_len // LANES

    def other(step):
        return lax.rem(walk + step, walk_count)

    def bulk(count, sem):
        view = spare.at[pl.ds(0, count)]
        return pltpu.make_async_remote_copy(
            src_ref=view, dst_ref=view, send_sem=sent, recv_sem=sem, device_id=(me, walk), device_id_type=MESH
        )

    barrier = pltpu.get_barrier_semaphore()

    def greet(peer):
        pl.semaphore_signal(
            barrier, inc=1, device_id=(peer // walk_count, lax.rem(peer, walk_count)), device_id_type=MESH
        )

    @pl.when(greets)
    def _():
        def greet_all(step, carry):
            greet(lax.rem(flat + step, total_count))
            return carry

        lax.fori_loop(1, total_count, greet_all, 0)

    @pl.when(jnp.logical_not(greets))
    def _():
        for step in range(1, walk_count):
            greet(me * walk_count + other(step))

    load(spare.at[pl.ds(0, load_rows)], spare.at[pl.ds(0, load_rows)], 0).wait()
    for copy in narrow:
        copy.wait()
    norm = norm_ref[0]
    walkers = walkers_ref[...]
    sq_h, sq_m, sq_l = split(walkers * walkers)
    wk_h, wk_m, wk_l = split(walkers)
    h, m, l = [sq_h, wk_h], [sq_m, wk_m], [sq_l, wk_l]
    one = jnp.ones((1, walk_len), F32)
    pad = jnp.zeros((LANES - 12 * dims - 8, walk_len), F32)
    stacked = jnp.concatenate(h + m + h + m + l + h + [row_of([one] * 3, walk_len), pad], 0)
    stacked = stacked.astype(BF16)
    width = 2 * LANES
    for quarter in range(quarters):
        walker_feat[quarter] = stacked[:, quarter * width : (quarter + 1) * width]

    centers = centers_ref[...]
    sigmas = sigmas_ref[...]
    inverse_var = 1.0 / (sigmas * sigmas)
    scaled = centers * inverse_var
    constant = jnp.log(heights_ref[...]) - 0.5 * jnp.sum(centers * scaled, 0, keepdims=True)
    k_sq = split((-0.5 * LOG2E) * inverse_var)
    k_lin = split(LOG2E * scaled)
    con = row_of(split(LOG2E * constant), shard_len)
    h, m, l = [[k_sq[i], k_lin[i]] for i in range(3)]
    pad = jnp.zeros((LANES - 12 * dims - 8, shard_len), F32)
    kernel_feat[...] = jnp.concatenate(h + h + m + m + h + l + [con, pad], 0).T.astype(BF16)

    live = live_ref[0]
    alive = (lax.broadcasted_iota(jnp.int32, (8, shard_len), 1) < live).astype(F32)
    mom_a = split(inverse_var * alive)
    mom_c = split(scaled * alive)
    pad = jnp.zeros((8, shard_len), F32)
    mom_rows = [mom_a[0], mom_c[0], mom_a[1], mom_c[1], mom_a[2], mom_c[2], row_of([alive], shard_len), pad]
    kernel_mom[...] = jnp.concatenate(mom_rows, 0).astype(BF16)

    live_row = jnp.full((1, LANES), live, jnp.int32).astype(F32)
    block = min(512, shard_len)

    def owner_of(quarter):
        return holders[quarter]

    def copy_a(quarter):
        return pltpu.make_async_remote_copy(
            src_ref=sums.at[quarter], dst_ref=got.at[me],
            send_sem=sent, recv_sem=recv_a,
            device_id=(owner_of(quarter), walk), device_id_type=MESH,
        )

    def copy_d(quarter):
        return pltpu.make_async_remote_copy(
            src_ref=sums.at[quarter], dst_ref=direct.at[me - 1, quarter - head],
            send_sem=sent, recv_sem=recv_d,
            device_id=(0, walk), device_id_type=MESH,
        )

    def copy_g(step, slot, quarter):
        return pltpu.make_async_remote_copy(
            src_ref=sums.at[quarter, :, pl.ds(dims, 1)], dst_ref=direct_far.at[walk, slot, quarter - head],
            send_sem=sent, recv_sem=recv_d,
            device_id=(0, other(step)), device_id_type=MESH,
        )

    def copy_b(target):
        return pltpu.make_async_remote_copy(
            src_ref=mine, dst_ref=shared.at[mine_quarter],
            send_sem=sent, recv_sem=recv_b,
            device_id=(target, walk), device_id_type=MESH,
        )

    def copy_c(step, target):
        return pltpu.make_async_remote_copy(
            src_ref=mine.at[:, pl.ds(dims, 1)], dst_ref=far.at[walk, mine_quarter],
            send_sem=sent, recv_sem=recv_b,
            device_id=(target, other(step)), device_id_type=MESH,
        )

    def copy_w(step, source):
        return (
            pltpu.make_async_remote_copy(
                src_ref=walkers_ref, dst_ref=far_walkers.at[source],
                send_sem=sent, recv_sem=recv_w,
                device_id=(me, other(step)), device_id_type=MESH,
            ),
            pltpu.make_async_remote_copy(
                src_ref=target_ref, dst_ref=far_targets.at[source],
                send_sem=sent, recv_sem=recv_w,
                device_id=(me, other(step)), device_id_type=MESH,
            ),
        )

    def compute(quarter):
        feat = walker_feat[quarter]
        moments = None
        for index in range(shard_len // block):
            part = slice(index * block, (index + 1) * block)
            e = jnp.exp2(jnp.dot(kernel_feat[part, :], feat, preferred_element_type=F32))
            high = e.astype(BF16)
            low = (e - high.astype(F32)).astype(BF16)
            moms = kernel_mom[:, part]
            add = jnp.dot(moms, high, preferred_element_type=F32) + jnp.dot(
                moms, low, preferred_element_type=F32
            )
            moments = add if moments is None else moments + add
        a_sum = moments[0:dims] + moments[2 * dims : 3 * dims] + moments[4 * dims : 5 * dims]
        c_sum = moments[dims : 2 * dims] + moments[3 * dims : 4 * dims] + moments[5 * dims : 6 * dims]
        density = moments[6 * dims : 6 * dims + 1]
        grad = c_sum - walkers_ref[:, quarter * width : (quarter + 1) * width] * a_sum
        for chunk in range(2):
            part = slice(chunk * LANES, (chunk + 1) * LANES)
            sums[quarter, chunk, 0:dims, :] = grad[:, part]
            sums[quarter, chunk, dims : dims + 1, :] = density[:, part]
            sums[quarter, chunk, dims + 1 : dims + 2, :] = live_row

    def send(quarter):
        if quarter >= head:
            @pl.when(me > 0)
            def _():
                copy_d(quarter).start()
                for step in range(1, walk_count):
                    copy_g(step, me - 1, quarter).start()

            @pl.when(me == 0)
            def _():
                for step in range(1, walk_count):
                    copy_g(step, kern_count - 1, quarter).start()

        @pl.when(me != owner_of(quarter))
        def _():
            copy_a(quarter).start()

    def enter():
        @pl.when(greets)
        def _():
            pl.semaphore_wait(barrier, greeted - 1)

        @pl.when(jnp.logical_not(greets))
        def _():
            pl.semaphore_wait(barrier, greeted + others)

    begin = 0
    for end in (quarters // 2, quarters):
        for quarter in range(begin, end):
            compute(quarter)

        @pl.when(me >= owners)
        def _():
            if begin == 0:
                enter()
            for quarter in range(begin, end):
                send(quarter)

        begin = end

    @pl.when(me < owners)
    def _():
        enter()
        for quarter in range(quarters):
            send(quarter)

    for step in range(1, walk_count):
        for copy in copy_w(step, walk):
            copy.start()

    far_walkers[walk] = walkers
    far_targets[walk] = target_ref[...]
    bulk(walker_rows, recv_w).wait_recv()
    targets = [far_targets[index] for index in range(walk_count)]
    if walk_count % 8:
        targets.append(jnp.full((8 - walk_count % 8, walk_len), -1, jnp.int32))
    local = jnp.concatenate(targets, 0) - me * shard_len
    owned = (local >= 0) & (local < shard_len)
    before = lax.broadcasted_iota(jnp.int32, (walk_len, walk_len), 0) < lax.broadcasted_iota(
        jnp.int32, (walk_len, walk_len), 1
    )
    place = jnp.dot(
        jnp.where(owned, 1.0, 0.0).astype(BF16),
        jnp.where(before, 1.0, 0.0).astype(BF16),
        preferred_element_type=F32,
    )
    slot = jnp.where(owned, (local + 1).astype(F32), 0.0)

    def pack(feat):
        return jnp.dot(feat.astype(BF16), table[...], preferred_element_type=F32)

    def of_walk(index, height):
        column = lax.broadcasted_iota(jnp.int32, (height, span), 1)
        return (column >= index * capacity) & (column < (index + 1) * capacity)

    span = walk_count * capacity
    lane = lax.broadcasted_iota(jnp.int32, (walk_len, LANES), 1).astype(F32)
    spots = [
        jnp.broadcast_to(jnp.where(owned[index : index + 1], place[index : index + 1] + index * capacity, -1.0), (LANES, walk_len)).T
        for index in range(walk_count)
    ]
    for at in range(0, span, LANES):
        hit = lane + at == spots[0]
        for spot in spots[1:]:
            hit = hit | (lane + at == spot)
        table[:, at : at + LANES] = jnp.where(hit, 1.0, 0.0).astype(BF16)
    packed = jnp.zeros((3 * dims + 8, span), F32)
    for index in range(walk_count):
        high, middle, low = split(far_walkers[index])
        slot_rows = row_of(split(slot[index : index + 1]), walk_len)
        found = pack(jnp.concatenate([high, middle, low, slot_rows], 0))
        packed = jnp.where(of_walk(index, 3 * dims + 8), found, packed)
    packed_walkers = packed[0:dims] + (packed[dims : 2 * dims] + packed[2 * dims : 3 * dims])
    at = 3 * dims
    packed_slot = packed[at : at + 1] + packed[at + 1 : at + 2] + packed[at + 2 : at + 3] - 1.0
    target_slot = jnp.broadcast_to(packed_slot, (LANES, span)).T
    lane = lax.broadcasted_iota(jnp.int32, (span, LANES), 1).astype(F32)
    for at in range(0, shard_len, LANES):
        placing[:, at : at + LANES] = jnp.where(lane + at == target_slot, 1.0, 0.0).astype(BF16)
    height = (3 * walk_count + 7) // 8 * 8
    row = lax.broadcasted_iota(jnp.int32, (height, span), 0)
    own = jnp.zeros((height, span), jnp.bool_)
    for index in range(walk_count):
        own = own | (of_walk(index, height) & (row >= 3 * index) & (row < 3 * index + 3))
    packed_squares = packed_walkers * packed_walkers

    def finish(total):
        live_total = total[dims + 1 : dims + 2]
        density = total[dims : dims + 1] / live_total
        ratio = density / norm + EPSILON
        return density, -PREFACTOR * (total[0:dims] / live_total) / (norm * ratio)

    def publish(total, begin):
        for chunk in range(2):
            density, force = finish(total[chunk])
            mine[chunk, 0:dims, :] = force
            mine[chunk, dims : dims + 1, :] = density
            shared[mine_quarter, chunk, 0:dims, :] = force
            shared[mine_quarter, chunk, dims : dims + 1, :] = density

        def start_b(target, carry):
            @pl.when(target != me)
            def _():
                copy_b(target).start()

            for step in range(1, walk_count):
                copy_c(step, target).start()
            return carry

        lax.fori_loop(begin, kern_count, start_b, 0)

    @pl.when(owns_head | owns_tail)
    def _():
        got[me] = sums[mine_quarter]
        bulk((kern_count - 1) * 2 * rows, recv_a).wait_recv()
        total = got[0]
        for source in range(1, kern_count):
            total = total + got[source]
        publish(total, jnp.where(owns_head, 0, 1))

    @pl.when(me == 0)
    def _():
        bulk(head * 2 * (dims + 1 + others), recv_b).wait_recv()
        bulk(DIRECT * 2 * ((kern_count - 1) * (rows + others) + others), recv_d).wait_recv()
        for index in range(DIRECT):
            whole = sums[head + index]
            for source in range(kern_count - 1):
                whole = whole + direct[source, index]
            for chunk in range(2):
                density, force = finish(whole[chunk])
                shared[head + index, chunk, 0:dims, :] = force
                shared[head + index, chunk, dims : dims + 1, :] = density
            for step in range(1, walk_count):
                origin = other(step)
                distant = direct_far[origin, 0, index]
                for source in range(1, kern_count):
                    distant = distant + direct_far[origin, source, index]
                for chunk in range(2):
                    far[origin, head + index, chunk] = distant[chunk] / whole[chunk, dims + 1 : dims + 2]

    @pl.when(owns_head | owns_tail)
    def _():
        bulk(2 * ((quarters - 1) * (dims + 1) + others * quarters), recv_b).wait_recv()

    @pl.when((me > 0) & jnp.logical_not(owns_head | owns_tail))
    def _():
        bulk(2 * (quarters * (dims + 1) + others * quarters), recv_b).wait_recv()

    def biased(density):
        return PREFACTOR * jnp.log(density / norm + EPSILON)

    for chunk in range(owners):
        part = slice(chunk * LANES, (chunk + 1) * LANES)
        density = shared[chunk // 2, chunk % 2, dims : dims + 1, :]
        far[walk, chunk // 2, chunk % 2] = density
        bias_ref[:, part] = biased(density)
        force_ref[:, part] = shared[chunk // 2, chunk % 2, 0:dims, :]
    density_sum = jnp.zeros((1, 1), F32)
    line = lax.broadcasted_iota(jnp.int32, (height, walk_len), 0)
    lines = jnp.zeros((height, walk_len), F32)
    for index in range(walk_count):
        whole = jnp.concatenate([far[index, chunk // 2, chunk % 2] for chunk in range(owners)], 1)
        density_sum = density_sum + jnp.sum(whole, 1, keepdims=True)
        for part, value in enumerate(split(whole)):
            lines = jnp.where(line == 3 * index + part, value, lines)
    weight = jnp.exp(biased(jnp.sum(jnp.where(own, pack(lines), 0.0), 0, keepdims=True)))
    lin = split(weight * packed_walkers)
    sq = split(weight * packed_squares)
    last = row_of(split(weight), span)
    pad = jnp.zeros((8, span), F32)
    feat = jnp.concatenate([lin[0], sq[0], lin[1], sq[1], lin[2], sq[2], last, pad], 0).astype(BF16)
    merged = jnp.dot(feat, placing[...], preferred_element_type=F32)
    log_norm = jnp.log((1.0 - RATE) * norm + RATE * density_sum / (walk_len * walk_count))
    bias_ref[:, walk_len : walk_len + LANES] = jnp.broadcast_to(log_norm, (1, LANES))

    first = merged[0:dims] + (merged[2 * dims : 3 * dims] + merged[4 * dims : 5 * dims])
    second = merged[dims : 2 * dims] + (merged[3 * dims : 4 * dims] + merged[5 * dims : 6 * dims])
    at = 6 * dims
    gain = merged[at : at + 1] + (merged[at + 1 : at + 2] + merged[at + 2 : at + 3])
    row = lax.broadcasted_iota(jnp.int32, (dims, dims), 0)
    column = lax.broadcasted_iota(jnp.int32, (dims, dims), 1)
    new_sigma = jnp.sum(jnp.where(row == column, new_sigma_ref[...], 0.0), 1, keepdims=True)
    centers = centers_ref[...]
    sigmas = sigmas_ref[...]
    heights = heights_ref[...]
    shift = first - centers * gain
    spread = second - 2.0 * centers * first + centers * centers * gain + new_sigma * new_sigma * gain
    new_heights = heights + gain
    inverse = 1.0 / new_heights
    delta = shift * inverse
    new_heights_ref[...] = new_heights
    new_centers_ref[...] = centers + delta
    new_sigmas_ref[...] = jnp.sqrt((heights * sigmas * sigmas + spread) * inverse - delta * delta)

    always = walker_rows + (quarters - 1) * 2 * rows
    direct_rows = DIRECT * 2 * (rows + others)

    @pl.when(owns_head)
    def _():
        bulk(always + direct_rows + 2 * ((kern_count - 1) * (dims + 1) + others * kern_count), sent).wait_send()

    @pl.when(owns_tail)
    def _():
        bulk(always + direct_rows + 2 * ((kern_count - 2) * (dims + 1) + others * (kern_count - 1)), sent).wait_send()

    @pl.when(me == 0)
    def _():
        bulk(always + 2 * rows + DIRECT * 2 * others, sent).wait_send()

    @pl.when((me > 0) & jnp.logical_not(owns_head | owns_tail))
    def _():
        bulk(always + 2 * rows + direct_rows, sent).wait_send()


def write_kernel(bias_ref, force_ref, new_heights_ref, new_centers_ref, new_sigmas_ref,
                 bias_hbm, force_hbm, new_heights_hbm, new_centers_hbm, new_sigmas_hbm, log_norm_hbm, log_norm_ref, sem):
    walk_len = bias_hbm.shape[1]
    log_norm_ref[...] = bias_ref[:, walk_len : walk_len + 1]
    pairs = [
        (new_centers_ref, new_centers_hbm),
        (new_sigmas_ref, new_sigmas_hbm),
        (force_ref, force_hbm),
        (new_heights_ref, new_heights_hbm),
        (bias_ref.at[:, pl.ds(0, walk_len)], bias_hbm),
        (log_norm_ref, log_norm_hbm),
    ]
    copies = [pltpu.make_async_copy(source, target, sem.at[index]) for index, (source, target) in enumerate(pairs)]
    for copy in copies:
        copy.start()
    for copy in copies:
        copy.wait()


def per_device(walkers, centers, sigmas, heights, kernel_live, merge_target, new_sigma, norm_old):
    dims, walk_len = walkers.shape
    shard_len = centers.shape[1]
    kern_count = lax.axis_size("kern")
    walk_count = lax.axis_size("walk")
    owners = walk_len // LANES
    quarters = owners // 2
    rows = dims + 2
    capacity = 2 * walk_len // kern_count
    height_row = heights.reshape(1, shard_len)
    load_rows = (dims * (walk_len + 2 * shard_len) + shard_len + walk_len) // LANES
    walker_rows = walk_count * (dims + 1) * walk_len // LANES
    answer_rows = 2 * kern_count * (walk_count + rows)
    spare_rows = load_rows + walker_rows + answer_rows + kern_count * owners * (rows + walk_count)

    dma = pltpu.SemaphoreType.DMA
    shapes = [(1, walk_len), (dims, walk_len), (1, shard_len), (dims, shard_len), (dims, shard_len), (1, 1)]
    results = pl.pallas_call(
        functools.partial(sums_kernel, kern_count, walk_count, owners, capacity),
        out_shape=[pltpu.VMEM(shape, F32) for shape in [(1, walk_len + LANES)] + shapes[1:5]],
        in_specs=[HBM] * 8,
        scratch_shapes=[
            pltpu.VMEM((dims, walk_len), F32),
            pltpu.VMEM((1, walk_len), jnp.int32),
            pltpu.VMEM((dims, shard_len), F32),
            pltpu.VMEM((dims, shard_len), F32),
            pltpu.VMEM((1, shard_len), F32),
            pltpu.SMEM((1,), jnp.int32),
            pltpu.SMEM((1,), F32),
            pltpu.VMEM((1, dims), F32),
            dma((4,)),
            pltpu.VMEM((walk_len // (2 * LANES), LANES, 2 * LANES), BF16),
            pltpu.VMEM((shard_len, LANES), BF16),
            pltpu.VMEM((6 * dims + 16, shard_len), BF16),
            pltpu.VMEM((quarters, 2, rows, LANES), F32),
            pltpu.VMEM((kern_count, 2, rows, LANES), F32),
            pltpu.VMEM((kern_count - 1, DIRECT, 2, rows, LANES), F32),
            pltpu.VMEM((walk_count, kern_count, DIRECT, 2, 1, LANES), F32),
            pltpu.VMEM((2, dims + 1, LANES), F32),
            pltpu.VMEM((quarters, 2, dims + 1, LANES), F32),
            pltpu.VMEM((walk_count, quarters, 2, 1, LANES), F32),
            pltpu.VMEM((walk_count, dims, walk_len), F32),
            pltpu.VMEM((walk_count, 1, walk_len), jnp.int32),
            pltpu.VMEM((walk_len, walk_count * capacity), BF16),
            pltpu.VMEM((walk_count * capacity, shard_len), BF16),
            pltpu.VMEM((spare_rows, LANES), F32),
            dma, dma, dma, dma, dma,
        ],
        compiler_params=pltpu.CompilerParams(collective_id=0, has_side_effects=True, vmem_limit_bytes=LIMIT),
        name="sums",
    )(*[
        pltpu.with_memory_space_constraint(x, pltpu.HBM)
        for x in (walkers, merge_target.reshape(1, walk_len), centers, sigmas, height_row)
    ], kernel_live, norm_old, pltpu.with_memory_space_constraint(new_sigma.reshape(1, dims), pltpu.HBM))

    bias, force, new_heights, new_centers, new_sigmas, log_norm = pl.pallas_call(
        write_kernel,
        out_shape=[jax.ShapeDtypeStruct(shape, F32) for shape in shapes],
        in_specs=[VMEM] * 5,
        out_specs=[HBM] * 6,
        scratch_shapes=[pltpu.VMEM((1, 1), F32), dma((6,))],
        compiler_params=pltpu.CompilerParams(vmem_limit_bytes=LIMIT),
        name="write",
    )(*results)
    return (bias.reshape(walk_len), force, new_heights.reshape(shard_len), new_centers, new_sigmas, log_norm.reshape(1))


def solution(mesh):
    in_specs = (
        P(None, "walk"),
        P(None, "kern"),
        P(None, "kern"),
        P("kern"),
        P("kern"),
        P("walk"),
        P(),
        P(),
    )
    out_specs = (P("walk"), P(None, "walk"), P("kern"), P(None, "kern"), P(None, "kern"), P())
    return jax.shard_map(
        per_device, mesh=mesh, in_specs=in_specs, out_specs=out_specs, check_vma=False
    )
```

```python
import functools
import math

import jax
import jax.numpy as jnp
from jax import lax
from jax.experimental import pallas as pl
from jax.experimental.pallas import tpu as pltpu
from jax.sharding import PartitionSpec as P

PREFACTOR = 0.9
EPSILON = 0.01
RATE = 0.25
LANES = 128
LOG2E = math.log2(math.e)
MESH = pl.DeviceIdType.MESH
F32 = jnp.float32
DIRECT = 2
BF16 = jnp.bfloat16
VMEM = pl.BlockSpec(memory_space=pltpu.VMEM)
HBM = pl.BlockSpec(memory_space=pltpu.HBM)
LIMIT = 24 << 20


def split(x):
    high = x.astype(BF16).astype(F32)
    rest = x - high
    middle = rest.astype(BF16).astype(F32)
    low = (rest - middle).astype(BF16).astype(F32)
    return high, middle, low


def row_of(parts, width):
    row = lax.broadcasted_iota(jnp.int32, (8, width), 0)
    block = jnp.zeros((8, width), F32)
    for index, part in enumerate(parts):
        block = jnp.where(row == index, part, block)
    return block


def sums_kernel(kern_count, walk_count, owners, capacity,
                walkers_hbm, target_hbm, centers_hbm, sigmas_hbm, heights_hbm, live_hbm, norm_hbm, new_sigma_hbm,
                bias_ref, force_ref, new_heights_ref, new_centers_ref, new_sigmas_ref,
                walkers_ref, target_ref, centers_ref, sigmas_ref, heights_ref, live_ref, norm_ref, new_sigma_ref, load_sem,
                walker_feat, kernel_feat, kernel_mom, sums, got, direct, direct_far,
                mine, shared, far, far_walkers, far_targets, table, placing, spare,
                sent, recv_a, recv_d, recv_b, recv_w):
    def load(source, target, index):
        return pltpu.make_async_copy(source, target, load_sem.at[index])

    wide = [
        load(walkers_hbm, walkers_ref, 0),
        load(centers_hbm, centers_ref, 0),
        load(sigmas_hbm, sigmas_ref, 0),
        load(heights_hbm, heights_ref, 0),
        load(target_hbm, target_ref, 0),
    ]
    narrow = [load(live_hbm, live_ref, 1), load(norm_hbm, norm_ref, 2), load(new_sigma_hbm, new_sigma_ref, 3)]
    for copy in wide + narrow:
        copy.start()
    dims, walk_len = walkers_ref.shape
    shard_len = centers_ref.shape[1]
    rows = dims + 2
    me = lax.axis_index("kern")
    walk = lax.axis_index("walk")
    flat = me * walk_count + walk
    total_count = kern_count * walk_count
    quarters = owners // 2
    head = quarters - DIRECT
    half = quarters // 2
    holders = [quarter + 1 for quarter in range(half)] + [
        kern_count - 1 - (quarter + 1 - half) * (kern_count // quarters) for quarter in range(half, quarters)
    ]
    mine_quarter = 0
    for quarter in range(1, quarters):
        mine_quarter = jnp.where(me == holders[quarter], quarter, mine_quarter)
    owns = me == holders[0]
    for holder in holders[1:]:
        owns = owns | (me == holder)
    owns_head = owns & (mine_quarter < head)
    owns_tail = owns & (mine_quarter >= head)
    greets = owns | (me == 0)
    greeted = (quarters + 1) * walk_count

    others = walk_count - 1
    load_rows = (dims * (walk_len + 2 * shard_len) + shard_len + walk_len) // LANES
    walker_rows = others * (dims + 1) * walk_len // LANES

    def other(step):
        return lax.rem(walk + step, walk_count)

    def bulk(count, sem):
        view = spare.at[pl.ds(0, count)]
        return pltpu.make_async_remote_copy(
            src_ref=view, dst_ref=view, send_sem=sent, recv_sem=sem, device_id=(me, walk), device_id_type=MESH
        )

    barrier = pltpu.get_barrier_semaphore()

    def greet(peer):
        pl.semaphore_signal(
            barrier, inc=1, device_id=(peer // walk_count, lax.rem(peer, walk_count)), device_id_type=MESH
        )

    @pl.when(greets)
    def _():
        def greet_all(step, carry):
            greet(lax.rem(flat + step, total_count))
            return carry

        lax.fori_loop(1, total_count, greet_all, 0)

    @pl.when(jnp.logical_not(greets))
    def _():
        for step in range(1, walk_count):
            greet(me * walk_count + other(step))

    load(spare.at[pl.ds(0, load_rows)], spare.at[pl.ds(0, load_rows)], 0).wait()
    for copy in narrow:
        copy.wait()
    norm = norm_ref[0]
    walkers = walkers_ref[...]
    sq_h, sq_m, sq_l = split(walkers * walkers)
    wk_h, wk_m, wk_l = split(walkers)
    h, m, l = [sq_h, wk_h], [sq_m, wk_m], [sq_l, wk_l]
    one = jnp.ones((1, walk_len), F32)
    pad = jnp.zeros((LANES - 12 * dims - 8, walk_len), F32)
    stacked = jnp.concatenate(h + m + h + m + l + h + [row_of([one] * 3, walk_len), pad], 0)
    stacked = stacked.astype(BF16)
    width = 2 * LANES
    for quarter in range(quarters):
        walker_feat[quarter] = stacked[:, quarter * width : (quarter + 1) * width]

    centers = centers_ref[...]
    sigmas = sigmas_ref[...]
    inverse_var = 1.0 / (sigmas * sigmas)
    scaled = centers * inverse_var
    constant = jnp.log(heights_ref[...]) - 0.5 * jnp.sum(centers * scaled, 0, keepdims=True)
    k_sq = split((-0.5 * LOG2E) * inverse_var)
    k_lin = split(LOG2E * scaled)
    con = row_of(split(LOG2E * constant), shard_len)
    h, m, l = [[k_sq[i], k_lin[i]] for i in range(3)]
    pad = jnp.zeros((LANES - 12 * dims - 8, shard_len), F32)
    kernel_feat[...] = jnp.concatenate(h + h + m + m + h + l + [con, pad], 0).T.astype(BF16)

    live = live_ref[0]
    alive = (lax.broadcasted_iota(jnp.int32, (8, shard_len), 1) < live).astype(F32)
    mom_a = split(inverse_var * alive)
    mom_c = split(scaled * alive)
    pad = jnp.zeros((8, shard_len), F32)
    mom_rows = [mom_a[0], mom_c[0], mom_a[1], mom_c[1], mom_a[2], mom_c[2], row_of([alive], shard_len), pad]
    kernel_mom[...] = jnp.concatenate(mom_rows, 0).astype(BF16)

    live_row = jnp.full((1, LANES), live, jnp.int32).astype(F32)
    block = min(512, shard_len)

    def owner_of(quarter):
        return holders[quarter]

    def copy_a(quarter):
        return pltpu.make_async_remote_copy(
            src_ref=sums.at[quarter], dst_ref=got.at[me],
            send_sem=sent, recv_sem=recv_a,
            device_id=(owner_of(quarter), walk), device_id_type=MESH,
        )

    def copy_d(quarter):
        return pltpu.make_async_remote_copy(
            src_ref=sums.at[quarter], dst_ref=direct.at[me - 1, quarter - head],
            send_sem=sent, recv_sem=recv_d,
            device_id=(0, walk), device_id_type=MESH,
        )

    def copy_g(step, slot, quarter):
        return pltpu.make_async_remote_copy(
            src_ref=sums.at[quarter, :, pl.ds(dims, 1)], dst_ref=direct_far.at[walk, slot, quarter - head],
            send_sem=sent, recv_sem=recv_d,
            device_id=(0, other(step)), device_id_type=MESH,
        )

    def copy_b(target):
        return pltpu.make_async_remote_copy(
            src_ref=mine, dst_ref=shared.at[mine_quarter],
            send_sem=sent, recv_sem=recv_b,
            device_id=(target, walk), device_id_type=MESH,
        )

    def copy_c(step, target):
        return pltpu.make_async_remote_copy(
            src_ref=mine.at[:, pl.ds(dims, 1)], dst_ref=far.at[walk, mine_quarter],
            send_sem=sent, recv_sem=recv_b,
            device_id=(target, other(step)), device_id_type=MESH,
        )

    def copy_w(step, source):
        return (
            pltpu.make_async_remote_copy(
                src_ref=walkers_ref, dst_ref=far_walkers.at[source],
                send_sem=sent, recv_sem=recv_w,
                device_id=(me, other(step)), device_id_type=MESH,
            ),
            pltpu.make_async_remote_copy(
                src_ref=target_ref, dst_ref=far_targets.at[source],
                send_sem=sent, recv_sem=recv_w,
                device_id=(me, other(step)), device_id_type=MESH,
            ),
        )

    def compute(quarter):
        feat = walker_feat[quarter]
        moments = None
        for index in range(shard_len // block):
            part = slice(index * block, (index + 1) * block)
            e = jnp.exp2(jnp.dot(kernel_feat[part, :], feat, preferred_element_type=F32))
            high = e.astype(BF16)
            low = (e - high.astype(F32)).astype(BF16)
            moms = kernel_mom[:, part]
            add = jnp.dot(moms, high, preferred_element_type=F32) + jnp.dot(
                moms, low, preferred_element_type=F32
            )
            moments = add if moments is None else moments + add
        a_sum = moments[0:dims] + moments[2 * dims : 3 * dims] + moments[4 * dims : 5 * dims]
        c_sum = moments[dims : 2 * dims] + moments[3 * dims : 4 * dims] + moments[5 * dims : 6 * dims]
        density = moments[6 * dims : 6 * dims + 1]
        grad = c_sum - walkers_ref[:, quarter * width : (quarter + 1) * width] * a_sum
        for chunk in range(2):
            part = slice(chunk * LANES, (chunk + 1) * LANES)
            sums[quarter, chunk, 0:dims, :] = grad[:, part]
            sums[quarter, chunk, dims : dims + 1, :] = density[:, part]
            sums[quarter, chunk, dims + 1 : dims + 2, :] = live_row

    def send(quarter):
        if quarter >= head:
            @pl.when(me > 0)
            def _():
                copy_d(quarter).start()
                for step in range(1, walk_count):
                    copy_g(step, me - 1, quarter).start()

            @pl.when(me == 0)
            def _():
                for step in range(1, walk_count):
                    copy_g(step, kern_count - 1, quarter).start()

        @pl.when(me != owner_of(quarter))
        def _():
            copy_a(quarter).start()

    def enter():
        @pl.when(greets)
        def _():
            pl.semaphore_wait(barrier, greeted - 1)

        @pl.when(jnp.logical_not(greets))
        def _():
            pl.semaphore_wait(barrier, greeted + others)

    begin = 0
    for end in (quarters // 2, quarters):
        for quarter in range(begin, end):
            compute(quarter)

        @pl.when(me >= owners)
        def _():
            if begin == 0:
                enter()
            for quarter in range(begin, end):
                send(quarter)

        begin = end

    @pl.when(me < owners)
    def _():
        enter()
        for quarter in range(quarters):
            send(quarter)

    for step in range(1, walk_count):
        for copy in copy_w(step, walk):
            copy.start()

    far_walkers[walk] = walkers
    far_targets[walk] = target_ref[...]
    bulk(walker_rows, recv_w).wait_recv()
    targets = [far_targets[index] for index in range(walk_count)]
    if walk_count % 8:
        targets.append(jnp.full((8 - walk_count % 8, walk_len), -1, jnp.int32))
    local = jnp.concatenate(targets, 0) - me * shard_len
    owned = (local >= 0) & (local < shard_len)
    before = lax.broadcasted_iota(jnp.int32, (walk_len, walk_len), 0) < lax.broadcasted_iota(
        jnp.int32, (walk_len, walk_len), 1
    )
    place = jnp.dot(
        jnp.where(owned, 1.0, 0.0).astype(BF16),
        jnp.where(before, 1.0, 0.0).astype(BF16),
        preferred_element_type=F32,
    )
    slot = jnp.where(owned, (local + 1).astype(F32), 0.0)

    def pack(feat):
        return jnp.dot(feat.astype(BF16), table[...], preferred_element_type=F32)

    def of_walk(index, height):
        column = lax.broadcasted_iota(jnp.int32, (height, span), 1)
        return (column >= index * capacity) & (column < (index + 1) * capacity)

    span = walk_count * capacity
    lane = lax.broadcasted_iota(jnp.int32, (walk_len, LANES), 1).astype(F32)
    spots = [
        jnp.broadcast_to(jnp.where(owned[index : index + 1], place[index : index + 1] + index * capacity, -1.0), (LANES, walk_len)).T
        for index in range(walk_count)
    ]
    for at in range(0, span, LANES):
        hit = lane + at == spots[0]
        for spot in spots[1:]:
            hit = hit | (lane + at == spot)
        table[:, at : at + LANES] = jnp.where(hit, 1.0, 0.0).astype(BF16)
    packed = jnp.zeros((3 * dims + 8, span), F32)
    for index in range(walk_count):
        high, middle, low = split(far_walkers[index])
        slot_rows = row_of(split(slot[index : index + 1]), walk_len)
        found = pack(jnp.concatenate([high, middle, low, slot_rows], 0))
        packed = jnp.where(of_walk(index, 3 * dims + 8), found, packed)
    packed_walkers = packed[0:dims] + (packed[dims : 2 * dims] + packed[2 * dims : 3 * dims])
    at = 3 * dims
    packed_slot = packed[at : at + 1] + packed[at + 1 : at + 2] + packed[at + 2 : at + 3] - 1.0
    target_slot = jnp.broadcast_to(packed_slot, (LANES, span)).T
    lane = lax.broadcasted_iota(jnp.int32, (span, LANES), 1).astype(F32)
    for at in range(0, shard_len, LANES):
        placing[:, at : at + LANES] = jnp.where(lane + at == target_slot, 1.0, 0.0).astype(BF16)
    height = (3 * walk_count + 7) // 8 * 8
    row = lax.broadcasted_iota(jnp.int32, (height, span), 0)
    own = jnp.zeros((height, span), jnp.bool_)
    for index in range(walk_count):
        own = own | (of_walk(index, height) & (row >= 3 * index) & (row < 3 * index + 3))
    packed_squares = packed_walkers * packed_walkers

    def finish(total):
        live_total = total[dims + 1 : dims + 2]
        density = total[dims : dims + 1] / live_total
        ratio = density / norm + EPSILON
        return density, -PREFACTOR * (total[0:dims] / live_total) / (norm * ratio)

    def publish(total, begin):
        for chunk in range(2):
            density, force = finish(total[chunk])
            mine[chunk, 0:dims, :] = force
            mine[chunk, dims : dims + 1, :] = density
            shared[mine_quarter, chunk, 0:dims, :] = force
            shared[mine_quarter, chunk, dims : dims + 1, :] = density

        def start_b(target, carry):
            @pl.when(target != me)
            def _():
                copy_b(target).start()

            for step in range(1, walk_count):
                copy_c(step, target).start()
            return carry

        lax.fori_loop(begin, kern_count, start_b, 0)

    @pl.when(owns_head | owns_tail)
    def _():
        got[me] = sums[mine_quarter]
        bulk((kern_count - 1) * 2 * rows, recv_a).wait_recv()
        total = got[0]
        for source in range(1, kern_count):
            total = total + got[source]
        publish(total, jnp.where(owns_head, 0, 1))

    @pl.when(me == 0)
    def _():
        bulk(DIRECT * 2 * ((kern_count - 1) * (rows + others) + others), recv_d).wait_recv()
        for index in range(DIRECT):
            whole = sums[head + index]
            for source in range(kern_count - 1):
                whole = whole + direct[source, index]
            for chunk in range(2):
                density, force = finish(whole[chunk])
                shared[head + index, chunk, 0:dims, :] = force
                shared[head + index, chunk, dims : dims + 1, :] = density
            for step in range(1, walk_count):
                origin = other(step)
                distant = direct_far[origin, 0, index]
                for source in range(1, kern_count):
                    distant = distant + direct_far[origin, source, index]
                for chunk in range(2):
                    far[origin, head + index, chunk] = distant[chunk] / whole[chunk, dims + 1 : dims + 2]
        bulk(head * 2 * (dims + 1 + others), recv_b).wait_recv()

    @pl.when(owns_head | owns_tail)
    def _():
        bulk(2 * ((quarters - 1) * (dims + 1) + others * quarters), recv_b).wait_recv()

    @pl.when((me > 0) & jnp.logical_not(owns_head | owns_tail))
    def _():
        bulk(2 * (quarters * (dims + 1) + others * quarters), recv_b).wait_recv()

    def biased(density):
        return PREFACTOR * jnp.log(density / norm + EPSILON)

    for chunk in range(owners):
        part = slice(chunk * LANES, (chunk + 1) * LANES)
        density = shared[chunk // 2, chunk % 2, dims : dims + 1, :]
        far[walk, chunk // 2, chunk % 2] = density
        bias_ref[:, part] = biased(density)
        force_ref[:, part] = shared[chunk // 2, chunk % 2, 0:dims, :]
    density_sum = jnp.zeros((1, 1), F32)
    line = lax.broadcasted_iota(jnp.int32, (height, walk_len), 0)
    lines = jnp.zeros((height, walk_len), F32)
    for index in range(walk_count):
        whole = jnp.concatenate([far[index, chunk // 2, chunk % 2] for chunk in range(owners)], 1)
        density_sum = density_sum + jnp.sum(whole, 1, keepdims=True)
        for part, value in enumerate(split(whole)):
            lines = jnp.where(line == 3 * index + part, value, lines)
    weight = jnp.exp(biased(jnp.sum(jnp.where(own, pack(lines), 0.0), 0, keepdims=True)))
    lin = split(weight * packed_walkers)
    sq = split(weight * packed_squares)
    last = row_of(split(weight), span)
    pad = jnp.zeros((8, span), F32)
    feat = jnp.concatenate([lin[0], sq[0], lin[1], sq[1], lin[2], sq[2], last, pad], 0).astype(BF16)
    merged = jnp.dot(feat, placing[...], preferred_element_type=F32)
    log_norm = jnp.log((1.0 - RATE) * norm + RATE * density_sum / (walk_len * walk_count))
    bias_ref[:, walk_len : walk_len + LANES] = jnp.broadcast_to(log_norm, (1, LANES))

    first = merged[0:dims] + (merged[2 * dims : 3 * dims] + merged[4 * dims : 5 * dims])
    second = merged[dims : 2 * dims] + (merged[3 * dims : 4 * dims] + merged[5 * dims : 6 * dims])
    at = 6 * dims
    gain = merged[at : at + 1] + (merged[at + 1 : at + 2] + merged[at + 2 : at + 3])
    row = lax.broadcasted_iota(jnp.int32, (dims, dims), 0)
    column = lax.broadcasted_iota(jnp.int32, (dims, dims), 1)
    new_sigma = jnp.sum(jnp.where(row == column, new_sigma_ref[...], 0.0), 1, keepdims=True)
    centers = centers_ref[...]
    sigmas = sigmas_ref[...]
    heights = heights_ref[...]
    shift = first - centers * gain
    spread = second - 2.0 * centers * first + centers * centers * gain + new_sigma * new_sigma * gain
    new_heights = heights + gain
    inverse = 1.0 / new_heights
    delta = shift * inverse
    new_heights_ref[...] = new_heights
    new_centers_ref[...] = centers + delta
    new_sigmas_ref[...] = jnp.sqrt((heights * sigmas * sigmas + spread) * inverse - delta * delta)

    always = walker_rows + (quarters - 1) * 2 * rows
    direct_rows = DIRECT * 2 * (rows + others)

    @pl.when(owns_head)
    def _():
        bulk(always + direct_rows + 2 * ((kern_count - 1) * (dims + 1) + others * kern_count), sent).wait_send()

    @pl.when(owns_tail)
    def _():
        bulk(always + direct_rows + 2 * ((kern_count - 2) * (dims + 1) + others * (kern_count - 1)), sent).wait_send()

    @pl.when(me == 0)
    def _():
        bulk(always + 2 * rows + DIRECT * 2 * others, sent).wait_send()

    @pl.when((me > 0) & jnp.logical_not(owns_head | owns_tail))
    def _():
        bulk(always + 2 * rows + direct_rows, sent).wait_send()


def write_kernel(bias_ref, force_ref, new_heights_ref, new_centers_ref, new_sigmas_ref,
                 bias_hbm, force_hbm, new_heights_hbm, new_centers_hbm, new_sigmas_hbm, log_norm_hbm, log_norm_ref, sem):
    walk_len = bias_hbm.shape[1]
    log_norm_ref[...] = bias_ref[:, walk_len : walk_len + 1]
    pairs = [
        (new_centers_ref, new_centers_hbm),
        (new_sigmas_ref, new_sigmas_hbm),
        (force_ref, force_hbm),
        (new_heights_ref, new_heights_hbm),
        (bias_ref.at[:, pl.ds(0, walk_len)], bias_hbm),
        (log_norm_ref, log_norm_hbm),
    ]
    copies = [pltpu.make_async_copy(source, target, sem.at[index]) for index, (source, target) in enumerate(pairs)]
    for copy in copies:
        copy.start()
    for copy in copies:
        copy.wait()


def per_device(walkers, centers, sigmas, heights, kernel_live, merge_target, new_sigma, norm_old):
    dims, walk_len = walkers.shape
    shard_len = centers.shape[1]
    kern_count = lax.axis_size("kern")
    walk_count = lax.axis_size("walk")
    owners = walk_len // LANES
    quarters = owners // 2
    rows = dims + 2
    capacity = 2 * walk_len // kern_count
    height_row = heights.reshape(1, shard_len)
    load_rows = (dims * (walk_len + 2 * shard_len) + shard_len + walk_len) // LANES
    walker_rows = walk_count * (dims + 1) * walk_len // LANES
    answer_rows = 2 * kern_count * (walk_count + rows)
    spare_rows = load_rows + walker_rows + answer_rows + kern_count * owners * (rows + walk_count)

    dma = pltpu.SemaphoreType.DMA
    shapes = [(1, walk_len), (dims, walk_len), (1, shard_len), (dims, shard_len), (dims, shard_len), (1, 1)]
    results = pl.pallas_call(
        functools.partial(sums_kernel, kern_count, walk_count, owners, capacity),
        out_shape=[pltpu.VMEM(shape, F32) for shape in [(1, walk_len + LANES)] + shapes[1:5]],
        in_specs=[HBM] * 8,
        scratch_shapes=[
            pltpu.VMEM((dims, walk_len), F32),
            pltpu.VMEM((1, walk_len), jnp.int32),
            pltpu.VMEM((dims, shard_len), F32),
            pltpu.VMEM((dims, shard_len), F32),
            pltpu.VMEM((1, shard_len), F32),
            pltpu.SMEM((1,), jnp.int32),
            pltpu.SMEM((1,), F32),
            pltpu.VMEM((1, dims), F32),
            dma((4,)),
            pltpu.VMEM((walk_len // (2 * LANES), LANES, 2 * LANES), BF16),
            pltpu.VMEM((shard_len, LANES), BF16),
            pltpu.VMEM((6 * dims + 16, shard_len), BF16),
            pltpu.VMEM((quarters, 2, rows, LANES), F32),
            pltpu.VMEM((kern_count, 2, rows, LANES), F32),
            pltpu.VMEM((kern_count - 1, DIRECT, 2, rows, LANES), F32),
            pltpu.VMEM((walk_count, kern_count, DIRECT, 2, 1, LANES), F32),
            pltpu.VMEM((2, dims + 1, LANES), F32),
            pltpu.VMEM((quarters, 2, dims + 1, LANES), F32),
            pltpu.VMEM((walk_count, quarters, 2, 1, LANES), F32),
            pltpu.VMEM((walk_count, dims, walk_len), F32),
            pltpu.VMEM((walk_count, 1, walk_len), jnp.int32),
            pltpu.VMEM((walk_len, walk_count * capacity), BF16),
            pltpu.VMEM((walk_count * capacity, shard_len), BF16),
            pltpu.VMEM((spare_rows, LANES), F32),
            dma, dma, dma, dma, dma,
        ],
        compiler_params=pltpu.CompilerParams(collective_id=0, has_side_effects=True, vmem_limit_bytes=LIMIT),
        name="sums",
    )(*[
        pltpu.with_memory_space_constraint(x, pltpu.HBM)
        for x in (walkers, merge_target.reshape(1, walk_len), centers, sigmas, height_row)
    ], kernel_live, norm_old, pltpu.with_memory_space_constraint(new_sigma.reshape(1, dims), pltpu.HBM))

    bias, force, new_heights, new_centers, new_sigmas, log_norm = pl.pallas_call(
        write_kernel,
        out_shape=[jax.ShapeDtypeStruct(shape, F32) for shape in shapes],
        in_specs=[VMEM] * 5,
        out_specs=[HBM] * 6,
        scratch_shapes=[pltpu.VMEM((1, 1), F32), dma((6,))],
        compiler_params=pltpu.CompilerParams(vmem_limit_bytes=LIMIT),
        name="write",
    )(*results)
    return (bias.reshape(walk_len), force, new_heights.reshape(shard_len), new_centers, new_sigmas, log_norm.reshape(1))


def solution(mesh):
    in_specs = (
        P(None, "walk"),
        P(None, "kern"),
        P(None, "kern"),
        P("kern"),
        P("kern"),
        P("walk"),
        P(),
        P(),
    )
    out_specs = (P("walk"), P(None, "walk"), P("kern"), P(None, "kern"), P(None, "kern"), P())
    return jax.shard_map(
        per_device, mesh=mesh, in_specs=in_specs, out_specs=out_specs, check_vma=False
    )
```

```python
import functools
import math

import jax
import jax.numpy as jnp
from jax import lax
from jax.experimental import pallas as pl
from jax.experimental.pallas import tpu as pltpu
from jax.sharding import PartitionSpec as P

PREFACTOR = 0.9
EPSILON = 0.01
RATE = 0.25
LANES = 128
LOG2E = math.log2(math.e)
MESH = pl.DeviceIdType.MESH
F32 = jnp.float32
DIRECT = 2
BF16 = jnp.bfloat16
VMEM = pl.BlockSpec(memory_space=pltpu.VMEM)
HBM = pl.BlockSpec(memory_space=pltpu.HBM)
LIMIT = 24 << 20


def split(x):
    high = x.astype(BF16).astype(F32)
    rest = x - high
    middle = rest.astype(BF16).astype(F32)
    low = (rest - middle).astype(BF16).astype(F32)
    return high, middle, low


def row_of(parts, width):
    row = lax.broadcasted_iota(jnp.int32, (8, width), 0)
    block = jnp.zeros((8, width), F32)
    for index, part in enumerate(parts):
        block = jnp.where(row == index, part, block)
    return block


def sums_kernel(kern_count, walk_count, owners, capacity,
                walkers_hbm, target_hbm, centers_hbm, sigmas_hbm, heights_hbm, live_hbm, norm_hbm, new_sigma_hbm,
                bias_ref, force_ref, new_heights_ref, new_centers_ref, new_sigmas_ref,
                walkers_ref, target_ref, centers_ref, sigmas_ref, heights_ref, live_ref, norm_ref, new_sigma_ref, load_sem,
                walker_feat, kernel_feat, kernel_mom, sums, got, direct, direct_far,
                mine, shared, far, far_walkers, far_targets, table, placing, spare,
                sent, recv_a, recv_d, recv_b, recv_w):
    def load(source, target, index):
        return pltpu.make_async_copy(source, target, load_sem.at[index])

    wide = [
        load(walkers_hbm, walkers_ref, 0),
        load(centers_hbm, centers_ref, 0),
        load(sigmas_hbm, sigmas_ref, 0),
        load(heights_hbm, heights_ref, 0),
        load(target_hbm, target_ref, 0),
    ]
    narrow = [load(live_hbm, live_ref, 1), load(norm_hbm, norm_ref, 2), load(new_sigma_hbm, new_sigma_ref, 3)]
    for copy in wide + narrow:
        copy.start()
    dims, walk_len = walkers_ref.shape
    shard_len = centers_ref.shape[1]
    rows = dims + 2
    me = lax.axis_index("kern")
    walk = lax.axis_index("walk")
    flat = me * walk_count + walk
    total_count = kern_count * walk_count
    quarters = owners // 2
    head = quarters - DIRECT
    half = quarters // 2
    holders = [quarter + 1 for quarter in range(half)] + [
        kern_count - 1 - (quarter + 1 - half) * (kern_count // quarters) for quarter in range(half, quarters)
    ]
    mine_quarter = 0
    for quarter in range(1, quarters):
        mine_quarter = jnp.where(me == holders[quarter], quarter, mine_quarter)
    owns = me == holders[0]
    for holder in holders[1:]:
        owns = owns | (me == holder)
    owns_head = owns & (mine_quarter < head)
    owns_tail = owns & (mine_quarter >= head)
    greets = owns | (me == 0)
    greeted = (quarters + 1) * walk_count

    others = walk_count - 1
    load_rows = (dims * (walk_len + 2 * shard_len) + shard_len + walk_len) // LANES
    walker_rows = others * (dims + 1) * walk_len // LANES

    def other(step):
        return lax.rem(walk + step, walk_count)

    def bulk(count, sem):
        view = spare.at[pl.ds(0, count)]
        return pltpu.make_async_remote_copy(
            src_ref=view, dst_ref=view, send_sem=sent, recv_sem=sem, device_id=(me, walk), device_id_type=MESH
        )

    barrier = pltpu.get_barrier_semaphore()

    def greet(peer):
        pl.semaphore_signal(
            barrier, inc=1, device_id=(peer // walk_count, lax.rem(peer, walk_count)), device_id_type=MESH
        )

    @pl.when(greets)
    def _():
        def greet_all(step, carry):
            greet(lax.rem(flat + step, total_count))
            return carry

        lax.fori_loop(1, total_count, greet_all, 0)

    @pl.when(jnp.logical_not(greets))
    def _():
        for step in range(1, walk_count):
            greet(me * walk_count + other(step))

    load(spare.at[pl.ds(0, load_rows)], spare.at[pl.ds(0, load_rows)], 0).wait()
    for copy in narrow:
        copy.wait()
    norm = norm_ref[0]
    walkers = walkers_ref[...]
    sq_h, sq_m, sq_l = split(walkers * walkers)
    wk_h, wk_m, wk_l = split(walkers)
    h, m, l = [sq_h, wk_h], [sq_m, wk_m], [sq_l, wk_l]
    one = jnp.ones((1, walk_len), F32)
    pad = jnp.zeros((LANES - 12 * dims - 8, walk_len), F32)
    stacked = jnp.concatenate(h + m + h + m + l + h + [row_of([one] * 3, walk_len), pad], 0)
    stacked = stacked.astype(BF16)
    width = 2 * LANES
    for quarter in range(quarters):
        walker_feat[quarter] = stacked[:, quarter * width : (quarter + 1) * width]

    centers = centers_ref[...]
    sigmas = sigmas_ref[...]
    inverse_var = 1.0 / (sigmas * sigmas)
    scaled = centers * inverse_var
    constant = jnp.log(heights_ref[...]) - 0.5 * jnp.sum(centers * scaled, 0, keepdims=True)
    k_sq = split((-0.5 * LOG2E) * inverse_var)
    k_lin = split(LOG2E * scaled)
    con = row_of(split(LOG2E * constant), shard_len)
    h, m, l = [[k_sq[i], k_lin[i]] for i in range(3)]
    pad = jnp.zeros((LANES - 12 * dims - 8, shard_len), F32)
    kernel_feat[...] = jnp.concatenate(h + h + m + m + h + l + [con, pad], 0).T.astype(BF16)

    live = live_ref[0]
    alive = (lax.broadcasted_iota(jnp.int32, (8, shard_len), 1) < live).astype(F32)
    mom_a = split(inverse_var * alive)
    mom_c = split(scaled * alive)
    pad = jnp.zeros((8, shard_len), F32)
    mom_rows = [mom_a[0], mom_c[0], mom_a[1], mom_c[1], mom_a[2], mom_c[2], row_of([alive], shard_len), pad]
    kernel_mom[...] = jnp.concatenate(mom_rows, 0).astype(BF16)

    live_row = jnp.full((1, LANES), live, jnp.int32).astype(F32)
    block = min(512, shard_len)

    def owner_of(quarter):
        return holders[quarter]

    def copy_a(quarter):
        return pltpu.make_async_remote_copy(
            src_ref=sums.at[quarter], dst_ref=got.at[me],
            send_sem=sent, recv_sem=recv_a,
            device_id=(owner_of(quarter), walk), device_id_type=MESH,
        )

    def copy_d(quarter):
        return pltpu.make_async_remote_copy(
            src_ref=sums.at[quarter], dst_ref=direct.at[me - 1, quarter - head],
            send_sem=sent, recv_sem=recv_d,
            device_id=(0, walk), device_id_type=MESH,
        )

    def copy_g(step, slot, quarter):
        return pltpu.make_async_remote_copy(
            src_ref=sums.at[quarter, :, pl.ds(dims, 1)], dst_ref=direct_far.at[walk, slot, quarter - head],
            send_sem=sent, recv_sem=recv_d,
            device_id=(0, other(step)), device_id_type=MESH,
        )

    def copy_b(target):
        return pltpu.make_async_remote_copy(
            src_ref=mine, dst_ref=shared.at[mine_quarter],
            send_sem=sent, recv_sem=recv_b,
            device_id=(target, walk), device_id_type=MESH,
        )

    def copy_c(step, target):
        return pltpu.make_async_remote_copy(
            src_ref=mine.at[:, pl.ds(dims, 1)], dst_ref=far.at[walk, mine_quarter],
            send_sem=sent, recv_sem=recv_b,
            device_id=(target, other(step)), device_id_type=MESH,
        )

    def copy_w(step, source):
        return (
            pltpu.make_async_remote_copy(
                src_ref=walkers_ref, dst_ref=far_walkers.at[source],
                send_sem=sent, recv_sem=recv_w,
                device_id=(me, other(step)), device_id_type=MESH,
            ),
            pltpu.make_async_remote_copy(
                src_ref=target_ref, dst_ref=far_targets.at[source],
                send_sem=sent, recv_sem=recv_w,
                device_id=(me, other(step)), device_id_type=MESH,
            ),
        )

    def compute(quarter):
        feat = walker_feat[quarter]
        moments = None
        for index in range(shard_len // block):
            part = slice(index * block, (index + 1) * block)
            e = jnp.exp2(jnp.dot(kernel_feat[part, :], feat, preferred_element_type=F32))
            high = e.astype(BF16)
            low = (e - high.astype(F32)).astype(BF16)
            moms = kernel_mom[:, part]
            add = jnp.dot(moms, high, preferred_element_type=F32) + jnp.dot(
                moms, low, preferred_element_type=F32
            )
            moments = add if moments is None else moments + add
        a_sum = moments[0:dims] + moments[2 * dims : 3 * dims] + moments[4 * dims : 5 * dims]
        c_sum = moments[dims : 2 * dims] + moments[3 * dims : 4 * dims] + moments[5 * dims : 6 * dims]
        density = moments[6 * dims : 6 * dims + 1]
        grad = c_sum - walkers_ref[:, quarter * width : (quarter + 1) * width] * a_sum
        for chunk in range(2):
            part = slice(chunk * LANES, (chunk + 1) * LANES)
            sums[quarter, chunk, 0:dims, :] = grad[:, part]
            sums[quarter, chunk, dims : dims + 1, :] = density[:, part]
            sums[quarter, chunk, dims + 1 : dims + 2, :] = live_row

    def send(quarter):
        if quarter >= head:
            @pl.when(me > 0)
            def _():
                copy_d(quarter).start()
                for step in range(1, walk_count):
                    copy_g(step, me - 1, quarter).start()

            @pl.when(me == 0)
            def _():
                for step in range(1, walk_count):
                    copy_g(step, kern_count - 1, quarter).start()

        @pl.when(me != owner_of(quarter))
        def _():
            copy_a(quarter).start()

    def enter():
        @pl.when(greets)
        def _():
            pl.semaphore_wait(barrier, greeted - 1)

        @pl.when(jnp.logical_not(greets))
        def _():
            pl.semaphore_wait(barrier, greeted + others)

    begin = 0
    for end in (quarters // 2, quarters):
        for quarter in range(begin, end):
            compute(quarter)

        @pl.when(me >= owners)
        def _():
            if begin == 0:
                enter()
            for quarter in range(begin, end):
                send(quarter)

        begin = end

    @pl.when(me < owners)
    def _():
        enter()
        for quarter in range(quarters):
            send(quarter)

    for step in range(1, walk_count):
        for copy in copy_w(step, walk):
            copy.start()

    far_walkers[walk] = walkers
    far_targets[walk] = target_ref[...]
    bulk(walker_rows, recv_w).wait_recv()
    targets = [far_targets[index] for index in range(walk_count)]
    if walk_count % 8:
        targets.append(jnp.full((8 - walk_count % 8, walk_len), -1, jnp.int32))
    local = jnp.concatenate(targets, 0) - me * shard_len
    owned = (local >= 0) & (local < shard_len)
    before = lax.broadcasted_iota(jnp.int32, (walk_len, walk_len), 0) < lax.broadcasted_iota(
        jnp.int32, (walk_len, walk_len), 1
    )
    place = jnp.dot(
        jnp.where(owned, 1.0, 0.0).astype(BF16),
        jnp.where(before, 1.0, 0.0).astype(BF16),
        preferred_element_type=F32,
    )
    slot = jnp.where(owned, (local + 1).astype(F32), 0.0)

    def pack(feat):
        return jnp.dot(feat.astype(BF16), table[...], preferred_element_type=F32)

    def of_walk(index, height):
        column = lax.broadcasted_iota(jnp.int32, (height, span), 1)
        return (column >= index * capacity) & (column < (index + 1) * capacity)

    span = walk_count * capacity
    lane = lax.broadcasted_iota(jnp.int32, (walk_len, LANES), 1).astype(F32)
    spots = [
        jnp.broadcast_to(jnp.where(owned[index : index + 1], place[index : index + 1] + index * capacity, -1.0), (LANES, walk_len)).T
        for index in range(walk_count)
    ]
    for at in range(0, span, LANES):
        hit = lane + at == spots[0]
        for spot in spots[1:]:
            hit = hit | (lane + at == spot)
        table[:, at : at + LANES] = jnp.where(hit, 1.0, 0.0).astype(BF16)
    packed = jnp.zeros((3 * dims + 8, span), F32)
    for index in range(walk_count):
        high, middle, low = split(far_walkers[index])
        slot_rows = row_of(split(slot[index : index + 1]), walk_len)
        found = pack(jnp.concatenate([high, middle, low, slot_rows], 0))
        packed = jnp.where(of_walk(index, 3 * dims + 8), found, packed)
    packed_walkers = packed[0:dims] + (packed[dims : 2 * dims] + packed[2 * dims : 3 * dims])
    at = 3 * dims
    packed_slot = packed[at : at + 1] + packed[at + 1 : at + 2] + packed[at + 2 : at + 3] - 1.0
    target_slot = jnp.broadcast_to(packed_slot, (LANES, span)).T
    lane = lax.broadcasted_iota(jnp.int32, (span, LANES), 1).astype(F32)
    for at in range(0, shard_len, LANES):
        placing[:, at : at + LANES] = jnp.where(lane + at == target_slot, 1.0, 0.0).astype(BF16)
    height = (3 * walk_count + 7) // 8 * 8
    row = lax.broadcasted_iota(jnp.int32, (height, span), 0)
    own = jnp.zeros((height, span), jnp.bool_)
    for index in range(walk_count):
        own = own | (of_walk(index, height) & (row >= 3 * index) & (row < 3 * index + 3))
    packed_squares = packed_walkers * packed_walkers

    def finish(total):
        live_total = total[dims + 1 : dims + 2]
        density = total[dims : dims + 1] / live_total
        ratio = density / norm + EPSILON
        return density, -PREFACTOR * (total[0:dims] / live_total) / (norm * ratio)

    def publish(total, begin):
        for chunk in range(2):
            density, force = finish(total[chunk])
            mine[chunk, 0:dims, :] = force
            mine[chunk, dims : dims + 1, :] = density
            shared[mine_quarter, chunk, 0:dims, :] = force
            shared[mine_quarter, chunk, dims : dims + 1, :] = density

        def start_b(target, carry):
            @pl.when(target != me)
            def _():
                copy_b(target).start()

            for step in range(1, walk_count):
                copy_c(step, target).start()
            return carry

        lax.fori_loop(begin, kern_count, start_b, 0)

    @pl.when(owns_head | owns_tail)
    def _():
        got[me] = sums[mine_quarter]
        bulk((kern_count - 1) * 2 * rows, recv_a).wait_recv()
        total = got[0]
        for source in range(1, kern_count):
            total = total + got[source]
        publish(total, jnp.where(owns_head, 0, 1))

    @pl.when(me == 0)
    def _():
        bulk(DIRECT * 2 * ((kern_count - 1) * (rows + others) + others), recv_d).wait_recv()
        for index in range(DIRECT):
            whole = sums[head + index]
            for source in range(kern_count - 1):
                whole = whole + direct[source, index]
            for chunk in range(2):
                density, force = finish(whole[chunk])
                shared[head + index, chunk, 0:dims, :] = force
                shared[head + index, chunk, dims : dims + 1, :] = density
            for step in range(1, walk_count):
                origin = other(step)
                distant = direct_far[origin, 0, index]
                for source in range(1, kern_count):
                    distant = distant + direct_far[origin, source, index]
                for chunk in range(2):
                    far[origin, head + index, chunk] = distant[chunk] / whole[chunk, dims + 1 : dims + 2]
        bulk(head * 2 * (dims + 1 + others), recv_b).wait_recv()

    @pl.when(owns_head | owns_tail)
    def _():
        bulk(2 * ((quarters - 1) * (dims + 1) + others * quarters), recv_b).wait_recv()

    @pl.when((me > 0) & jnp.logical_not(owns_head | owns_tail))
    def _():
        bulk(2 * (quarters * (dims + 1) + others * quarters), recv_b).wait_recv()

    def biased(density):
        return PREFACTOR * jnp.log(density / norm + EPSILON)

    for chunk in range(owners):
        part = slice(chunk * LANES, (chunk + 1) * LANES)
        density = shared[chunk // 2, chunk % 2, dims : dims + 1, :]
        far[walk, chunk // 2, chunk % 2] = density
        bias_ref[:, part] = biased(density)
        force_ref[:, part] = shared[chunk // 2, chunk % 2, 0:dims, :]
    density_sum = jnp.zeros((1, 1), F32)
    line = lax.broadcasted_iota(jnp.int32, (height, walk_len), 0)
    lines = jnp.zeros((height, walk_len), F32)
    for index in range(walk_count):
        whole = jnp.concatenate([far[index, chunk // 2, chunk % 2] for chunk in range(owners)], 1)
        density_sum = density_sum + jnp.sum(whole, 1, keepdims=True)
        for part, value in enumerate(split(whole)):
            lines = jnp.where(line == 3 * index + part, value, lines)
    weight = jnp.exp(biased(jnp.sum(jnp.where(own, pack(lines), 0.0), 0, keepdims=True)))
    lin = split(weight * packed_walkers)
    sq = split(weight * packed_squares)
    last = row_of(split(weight), span)
    pad = jnp.zeros((8, span), F32)
    feat = jnp.concatenate([lin[0], sq[0], lin[1], sq[1], lin[2], sq[2], last, pad], 0).astype(BF16)
    merged = jnp.dot(feat, placing[...], preferred_element_type=F32)
    log_norm = jnp.log((1.0 - RATE) * norm + RATE * density_sum / (walk_len * walk_count))
    bias_ref[:, walk_len : walk_len + LANES] = jnp.broadcast_to(log_norm, (1, LANES))

    first = merged[0:dims] + (merged[2 * dims : 3 * dims] + merged[4 * dims : 5 * dims])
    second = merged[dims : 2 * dims] + (merged[3 * dims : 4 * dims] + merged[5 * dims : 6 * dims])
    at = 6 * dims
    gain = merged[at : at + 1] + (merged[at + 1 : at + 2] + merged[at + 2 : at + 3])
    row = lax.broadcasted_iota(jnp.int32, (dims, dims), 0)
    column = lax.broadcasted_iota(jnp.int32, (dims, dims), 1)
    new_sigma = jnp.sum(jnp.where(row == column, new_sigma_ref[...], 0.0), 1, keepdims=True)
    centers = centers_ref[...]
    sigmas = sigmas_ref[...]
    heights = heights_ref[...]
    shift = first - centers * gain
    spread = second - 2.0 * centers * first + centers * centers * gain + new_sigma * new_sigma * gain
    new_heights = heights + gain
    inverse = 1.0 / new_heights
    delta = shift * inverse
    new_heights_ref[...] = new_heights
    new_centers_ref[...] = centers + delta
    new_sigmas_ref[...] = jnp.sqrt((heights * sigmas * sigmas + spread) * inverse - delta * delta)

    always = walker_rows + (quarters - 1) * 2 * rows
    direct_rows = DIRECT * 2 * (rows + others)

    @pl.when(owns_head)
    def _():
        bulk(always + direct_rows + 2 * ((kern_count - 1) * (dims + 1) + others * kern_count), sent).wait_send()

    @pl.when(owns_tail)
    def _():
        bulk(always + direct_rows + 2 * ((kern_count - 2) * (dims + 1) + others * (kern_count - 1)), sent).wait_send()

    @pl.when(me == 0)
    def _():
        bulk(always + 2 * rows + DIRECT * 2 * others, sent).wait_send()

    @pl.when((me > 0) & jnp.logical_not(owns_head | owns_tail))
    def _():
        bulk(always + 2 * rows + direct_rows, sent).wait_send()


def write_kernel(bias_ref, force_ref, new_heights_ref, new_centers_ref, new_sigmas_ref,
                 bias_hbm, force_hbm, new_heights_hbm, new_centers_hbm, new_sigmas_hbm, log_norm_hbm, log_norm_ref, spare, sem):
    walk_len = bias_hbm.shape[1]
    log_norm_ref[...] = bias_ref[:, walk_len : walk_len + 1]
    pairs = [
        (new_centers_ref, new_centers_hbm),
        (new_sigmas_ref, new_sigmas_hbm),
        (force_ref, force_hbm),
        (new_heights_ref, new_heights_hbm),
        (bias_ref.at[:, pl.ds(0, walk_len)], bias_hbm),
        (log_norm_ref, log_norm_hbm),
    ]
    copies = [pltpu.make_async_copy(source, target, sem.at[index // 5]) for index, (source, target) in enumerate(pairs)]
    for copy in copies:
        copy.start()
    pltpu.make_async_copy(spare, spare, sem.at[0]).wait()
    copies[5].wait()


def per_device(walkers, centers, sigmas, heights, kernel_live, merge_target, new_sigma, norm_old):
    dims, walk_len = walkers.shape
    shard_len = centers.shape[1]
    kern_count = lax.axis_size("kern")
    walk_count = lax.axis_size("walk")
    owners = walk_len // LANES
    quarters = owners // 2
    rows = dims + 2
    capacity = 2 * walk_len // kern_count
    height_row = heights.reshape(1, shard_len)
    load_rows = (dims * (walk_len + 2 * shard_len) + shard_len + walk_len) // LANES
    walker_rows = walk_count * (dims + 1) * walk_len // LANES
    answer_rows = 2 * kern_count * (walk_count + rows)
    spare_rows = load_rows + walker_rows + answer_rows + kern_count * owners * (rows + walk_count)

    dma = pltpu.SemaphoreType.DMA
    shapes = [(1, walk_len), (dims, walk_len), (1, shard_len), (dims, shard_len), (dims, shard_len), (1, 1)]
    results = pl.pallas_call(
        functools.partial(sums_kernel, kern_count, walk_count, owners, capacity),
        out_shape=[pltpu.VMEM(shape, F32) for shape in [(1, walk_len + LANES)] + shapes[1:5]],
        in_specs=[HBM] * 8,
        scratch_shapes=[
            pltpu.VMEM((dims, walk_len), F32),
            pltpu.VMEM((1, walk_len), jnp.int32),
            pltpu.VMEM((dims, shard_len), F32),
            pltpu.VMEM((dims, shard_len), F32),
            pltpu.VMEM((1, shard_len), F32),
            pltpu.SMEM((1,), jnp.int32),
            pltpu.SMEM((1,), F32),
            pltpu.VMEM((1, dims), F32),
            dma((4,)),
            pltpu.VMEM((walk_len // (2 * LANES), LANES, 2 * LANES), BF16),
            pltpu.VMEM((shard_len, LANES), BF16),
            pltpu.VMEM((6 * dims + 16, shard_len), BF16),
            pltpu.VMEM((quarters, 2, rows, LANES), F32),
            pltpu.VMEM((kern_count, 2, rows, LANES), F32),
            pltpu.VMEM((kern_count - 1, DIRECT, 2, rows, LANES), F32),
            pltpu.VMEM((walk_count, kern_count, DIRECT, 2, 1, LANES), F32),
            pltpu.VMEM((2, dims + 1, LANES), F32),
            pltpu.VMEM((quarters, 2, dims + 1, LANES), F32),
            pltpu.VMEM((walk_count, quarters, 2, 1, LANES), F32),
            pltpu.VMEM((walk_count, dims, walk_len), F32),
            pltpu.VMEM((walk_count, 1, walk_len), jnp.int32),
            pltpu.VMEM((walk_len, walk_count * capacity), BF16),
            pltpu.VMEM((walk_count * capacity, shard_len), BF16),
            pltpu.VMEM((spare_rows, LANES), F32),
            dma, dma, dma, dma, dma,
        ],
        compiler_params=pltpu.CompilerParams(collective_id=0, has_side_effects=True, vmem_limit_bytes=LIMIT),
        name="sums",
    )(*[
        pltpu.with_memory_space_constraint(x, pltpu.HBM)
        for x in (walkers, merge_target.reshape(1, walk_len), centers, sigmas, height_row)
    ], kernel_live, norm_old, pltpu.with_memory_space_constraint(new_sigma.reshape(1, dims), pltpu.HBM))

    bias, force, new_heights, new_centers, new_sigmas, log_norm = pl.pallas_call(
        write_kernel,
        out_shape=[jax.ShapeDtypeStruct(shape, F32) for shape in shapes],
        in_specs=[VMEM] * 5,
        out_specs=[HBM] * 6,
        scratch_shapes=[pltpu.VMEM((1, 1), F32), pltpu.VMEM((load_rows, LANES), F32), dma((2,))],
        compiler_params=pltpu.CompilerParams(vmem_limit_bytes=LIMIT),
        name="write",
    )(*results)
    return (bias.reshape(walk_len), force, new_heights.reshape(shard_len), new_centers, new_sigmas, log_norm.reshape(1))


def solution(mesh):
    in_specs = (
        P(None, "walk"),
        P(None, "kern"),
        P(None, "kern"),
        P("kern"),
        P("kern"),
        P("walk"),
        P(),
        P(),
    )
    out_specs = (P("walk"), P(None, "walk"), P("kern"), P(None, "kern"), P(None, "kern"), P())
    return jax.shard_map(
        per_device, mesh=mesh, in_specs=in_specs, out_specs=out_specs, check_vma=False
    )
```
